32 devices in a mesh: fsdp: 8 (over z, x), context: 2 (over y), tensor: 2 (over core).
Axes of the slice: x: 2, y: 2, z: 4, core: 2. Of those that a mesh axis runs over, the one named last changes fastest.
Arguments:
- tokens: bfloat16 [16, 640, 1024], P('fsdp', 'context'), may hold values from -6 to 6
- segments: int32 [16, 640], P('fsdp'), may hold values from 0 to 1, as said below
- first_gain: float32 [1024], replicated, may hold values from 0.1 to 1.9
- first_shift: float32 [1024], replicated, may hold values from -4 to 4
- input_weight: bfloat16 [1024, 3, 1024], P(('fsdp', 'context'), None, 'tensor'), may hold values from -0.1875 to 0.1875
- input_bias: float32 [2, 1024], P(None, 'tensor'), may hold values from -6 to 6
- output_weight: bfloat16 [1024, 1024], P(('fsdp', 'context'), 'tensor'), may hold values from -2.5 to 2.5
- output_bias: float32 [2, 1024], replicated, may hold values from -6 to 6
- second_gain: float32 [1024], replicated, may hold values from 0.1 to 1.9
- second_shift: float32 [1024], replicated, may hold values from -4 to 4
- up_weight: bfloat16 [1024, 4096], P(('fsdp', 'context'), 'tensor'), may hold values from -0.1875 to 0.1875
- up_bias: float32 [4096], P('tensor'), may hold values from -6 to 6
- down_weight: bfloat16 [1024, 4096], P(('fsdp', 'context'), 'tensor'), may hold values from -0.09375 to 0.09375
- cotangent: bfloat16 [16, 640, 1024], P('fsdp', 'context'), may hold values from -6 to 6
Outputs:
- block_output: bfloat16 [16, 640, 1024], P('fsdp', 'context')
- tokens_gradient: float32 [16, 640, 1024], P('fsdp', 'context')
- first_gain_gradient: float32 [1024], replicated
- first_shift_gradient: float32 [1024], replicated
- input_weight_gradient: float32 [1024, 3, 1024], P(('fsdp', 'context'), None, 'tensor')
- input_bias_gradient: float32 [2, 1024], P(None, 'tensor')
- output_weight_gradient: float32 [1024, 1024], P(('fsdp', 'context'), 'tensor')
- output_bias_gradient: float32 [2, 1024], replicated
- second_gain_gradient: float32 [1024], replicated
- second_shift_gradient: float32 [1024], replicated
- up_weight_gradient: float32 [1024, 4096], P(('fsdp', 'context'), 'tensor')
- up_bias_gradient: float32 [4096], P('tensor')
- down_weight_gradient: float32 [1024, 4096], P(('fsdp', 'context'), 'tensor')
- clipped_weight: float32 [1024, 2, 1024], P(('fsdp', 'context'), None, 'tensor')
- clip_factor: float32 [16], P('tensor')
The draws below stay inside these ranges and needn't reach their ends.
Inputs may be any that keep to these rules, and one draw needn't show every extreme that they name: `segments`: each row of 640 slots holds one image: 577 consecutive slots with segment number 1, starting at a drawn offset; all other slots are 0.
All inputs are finite; a program needn't handle non-finite values.
Results may differ from the reference program's by a relative error of at most 0.014.
Values may be sent and summed in bfloat16 or wider, within the bound.
A program may use at most 128 MiB of HBM per device.

```python
import jax
import jax.numpy as jnp
from jax import lax

D = 1024
FF = 4096
HEADS = 16
HEAD_DIM = 64
IMAGE = 577
ROW = 640
ROWS = 16


def draw_segments(key, part):
    offsets = jax.random.randint(jax.random.fold_in(key, 11), (ROWS,), 0, ROW - IMAGE + 1).astype(jnp.int32)
    slots = jnp.arange(ROW, dtype=jnp.int32)
    inside = (slots[None, :] >= offsets[:, None]) & (slots[None, :] < offsets[:, None] + IMAGE)
    return inside.astype(jnp.int32)


def block_levels(own_key, dims, shards, least, largest):
    level, own = 1.0, jax.random.fold_in(own_key, 6)
    for dim, parts in shards:
        steps = jnp.exp(jax.random.uniform(jax.random.fold_in(own, dim), (parts,), jnp.float32, least / len(shards), largest / len(shards)))
        level = level * jnp.repeat(steps, dims[dim] // parts).reshape([-1 if axis == dim else 1 for axis in range(len(dims))])
    return level


def bell_draw(rng, extent, deviation, bound, pieces=(), held_as=jnp.bfloat16):
    level = block_levels(rng, extent, pieces, -0.22, 0.18) if pieces else 1.0
    entries = jax.random.normal(rng, extent, jnp.float32) * deviation * level
    return jnp.minimum(jnp.maximum(entries, -bound), bound).astype(held_as)


def setup_inputs(seed: int = 0) -> dict:
    key_list = jax.random.split(jax.random.key(seed), 15)
    tokens = bell_draw(key_list[0], (ROWS, ROW, D), 1.0, 6.0, ((0, 8), (1, 2)))
    segments = draw_segments(jax.random.fold_in(key_list[14], 71), 0)
    first_gain = jnp.clip(1.0 + 0.18 * jax.random.normal(key_list[2], (D,), jnp.float32), 0.1, 1.9)
    first_shift = bell_draw(key_list[3], (D,), 0.3, 4.0, (), jnp.float32)
    input_weight = bell_draw(key_list[4], (D, 3, D), D ** -0.5, 0.1875, ((0, 16), (2, 2)))
    input_bias = bell_draw(key_list[5], (2, D), 0.5, 6.0, ((1, 2),), jnp.float32)
    output_weight = bell_draw(key_list[6], (D, D), (max(1, 3 * D // IMAGE)) ** -0.5, 2.5, ((0, 16), (1, 2)))
    output_bias = bell_draw(key_list[7], (2, D), 0.5, 6.0, (), jnp.float32)
    second_gain = jnp.clip(1.0 + 0.18 * jax.random.normal(key_list[8], (D,), jnp.float32), 0.1, 1.9)
    second_shift = bell_draw(key_list[9], (D,), 0.3, 4.0, (), jnp.float32)
    up_weight = bell_draw(key_list[10], (D, FF), D ** -0.5, 0.1875, ((0, 16), (1, 2)))
    up_bias = bell_draw(key_list[11], (FF,), 0.5, 6.0, ((0, 2),), jnp.float32)
    down_weight = bell_draw(key_list[12], (D, FF), FF ** -0.5, 0.09375, ((0, 16), (1, 2)))
    cotangent = bell_draw(key_list[13], (ROWS, ROW, D), 1.0, 6.0, ((0, 8), (1, 2)))
    return {"tokens": tokens, "segments": segments, "first_gain": first_gain, "first_shift": first_shift, "input_weight": input_weight, "input_bias": input_bias, "output_weight": output_weight, "output_bias": output_bias, "second_gain": second_gain, "second_shift": second_shift, "up_weight": up_weight, "up_bias": up_bias, "down_weight": down_weight, "cotangent": cotangent}


@jax.custom_vjp
def low(v):
    return lax.optimization_barrier(v.astype(jnp.bfloat16)).astype(jnp.float32)

@jax.custom_vjp
def low_back(v):
    return v

def low_keep(v):
    return (low(v), None)

def low_pass(kept, grad):
    return (grad,)

def back_keep(v):
    return (v, None)

def back_low(kept, grad):
    return (low(grad),)
low.defvjp(low_keep, low_pass)
low_back.defvjp(back_keep, back_low)
EPSILON = 1e-06
CLIP_LIMIT = 1.5
MASKED = -1e+30
HIGHEST = lax.Precision.HIGHEST

def normalize(values, gain, shift):
    average = lax.optimization_barrier(jnp.mean(values, axis=-1, keepdims=True))
    centered = values - average
    variance = lax.optimization_barrier(jnp.mean(centered * centered, axis=-1, keepdims=True))
    return centered * lax.rsqrt(variance + EPSILON) * gain + shift

def layer_row(params, row_tokens, row_segments):
    first_gain, first_shift, input_weight, input_bias, output_weight, output_bias, second_gain, second_shift, up_weight, up_bias, down_weight = params
    slots = row_tokens.shape[0]
    first_operand = low(normalize(row_tokens, first_gain, first_shift))
    projected = jnp.einsum('td,dcf->tcf', first_operand, input_weight, precision=HIGHEST)
    query = low_back(low(projected[:, 0] + input_bias[0]))
    key_part = low_back(low(projected[:, 1]))
    value_part = low_back(low(projected[:, 2] + input_bias[1]))
    query_heads = query.reshape(slots, HEADS, HEAD_DIM)
    key_heads = key_part.reshape(slots, HEADS, HEAD_DIM)
    value_heads = value_part.reshape(slots, HEADS, HEAD_DIM)
    raw_scores = low_back(jnp.einsum('qhd,khd->hqk', query_heads, key_heads, precision=HIGHEST))
    logits = raw_scores * HEAD_DIM ** (-0.5)
    allowed = row_segments[None, :] == row_segments[:, None]
    real_pairs = allowed & (row_segments[:, None] > 0)
    probs = jax.nn.softmax(jnp.where(allowed[None], logits, MASKED), axis=-1)
    peaks = lax.optimization_barrier(jnp.max(jnp.where(real_pairs[None], logits, MASKED), axis=(1, 2)))
    context = jnp.einsum('hqk,khd->qhd', low(probs), value_heads, precision=HIGHEST).reshape(slots, D)
    context = low_back(low(context))
    attended = low_back(jnp.dot(context, output_weight.T, precision=HIGHEST)) + output_bias[0]
    residual = row_tokens + attended
    second_operand = low(normalize(residual, second_gain, second_shift))
    pre_act = low_back(jnp.dot(second_operand, up_weight, precision=HIGHEST) + up_bias)
    hidden = low(jax.nn.gelu(pre_act, approximate=False))
    mixed = low_back(jnp.dot(hidden, down_weight.T, precision=HIGHEST)) + output_bias[1]
    keep_rows = (row_segments > 0)[:, None].astype(jnp.float32)
    return ((residual + mixed) * keep_rows, peaks)

def forward(all_tokens, params, segments):
    checked = jax.checkpoint(layer_row)

    def step(carry, items):
        result, peaks = checked(params, items[0], items[1])
        return (carry, (result, peaks))
    start = jnp.zeros((), jnp.float32)
    unused, (results, peaks) = lax.scan(step, start, (all_tokens, segments))
    return (results, lax.optimization_barrier(jnp.max(peaks, axis=0)))

def reference(tokens, segments, first_gain, first_shift, input_weight, input_bias, output_weight, output_bias, second_gain, second_shift, up_weight, up_bias, down_weight, cotangent):
    weights = (first_gain, first_shift, input_weight, input_bias, output_weight, output_bias, second_gain, second_shift, up_weight, up_bias, down_weight)
    weights = tuple((entry.astype(jnp.float32) for entry in weights))

    def wrapped(tokens_float, *params):
        return forward(tokens_float, params, segments)
    result, pullback, peaks = jax.vjp(wrapped, tokens.astype(jnp.float32), *weights, has_aux=True)
    grads = pullback(cotangent.astype(jnp.float32))
    factor = CLIP_LIMIT / jnp.maximum(peaks, CLIP_LIMIT)
    column_scale = jnp.repeat(jnp.sqrt(factor), HEAD_DIM)
    clipped = weights[2][:, :2, :] * column_scale[None, None, :]
    return (result.astype(jnp.bfloat16), grads[0], grads[1], grads[2], grads[3], grads[4], grads[5], grads[6], grads[7], grads[8], grads[9], grads[10], grads[11], clipped, factor)
```

```python
import functools

import jax
import jax.numpy as jnp
from jax import lax
from jax.experimental import pallas as pl
from jax.experimental.pallas import tpu as pltpu
from jax.sharding import PartitionSpec as P

HEAD_DIM = 64


EPSILON = 1e-06
CLIP_LIMIT = 1.5
MASKED = -1e30
HALF_ROOT = 0.7071067811865476
DENSITY = 0.3989422804014327


def normalize(values, gain, shift):
    average = jnp.mean(values, axis=-1, keepdims=True)
    centered = values - average
    inverse = lax.rsqrt(jnp.mean(centered * centered, axis=-1, keepdims=True) + EPSILON)
    scaled = centered * inverse
    return (scaled * gain + shift, scaled, inverse)


def normalize_back(incoming, scaled, inverse, gain):
    weighted = incoming * gain
    bracket = (
        weighted
        - jnp.mean(weighted, axis=-1, keepdims=True)
        - scaled * jnp.mean(weighted * scaled, axis=-1, keepdims=True)
    )
    return (inverse * bracket, jnp.sum(incoming * scaled, axis=0), jnp.sum(incoming, axis=0))


def gelu_slope(values):
    return (
        0.5 * (1.0 + lax.erf(values * HALF_ROOT))
        + values * jnp.exp(-0.5 * values * values) * DENSITY
    )


def split_heads(values):
    shaped = values.reshape(values.shape[0], values.shape[1], -1, HEAD_DIM)
    return jnp.transpose(shaped, (2, 0, 1, 3))


def join_heads(values):
    moved = jnp.transpose(values, (1, 2, 0, 3))
    return moved.reshape(moved.shape[0], moved.shape[1], -1)


BF = jnp.bfloat16
F32 = jnp.float32
COLS = 512
TILE = 256
PIECES = 12
BIG = 1e30
MESH_ID = pl.DeviceIdType.MESH


def nn(left, right):
    return jnp.dot(left, right, preferred_element_type=F32)


def nt(left, right):
    return lax.dot_general(left, right, (((1,), (1,)), ((), ())), preferred_element_type=F32)


def loop(count, body, start=0):
    def step(index, carry):
        body(index)
        return carry

    lax.fori_loop(start, count, step, 0)


def part(index, size):
    return pl.ds(pl.multiple_of(index * size, size), size)


def fold(block):
    return jnp.sum(block.reshape(-1, 8, block.shape[-1]), axis=0)


def layer_kernel(
    chain,
    tokens,
    cotangent,
    weight_in,
    weight_out,
    weight_up,
    weight_down,
    first_gain,
    first_shift,
    bias_three,
    output_bias,
    second_gain,
    second_shift,
    up_bias,
    keep_col,
    keep_row,
    block_out,
    token_grad,
    in_sum,
    out_sum,
    up_sum,
    down_sum,
    small_out,
    peak_out,
    store,
    near,
    mid,
    far,
    row_in,
    row_up,
    plain,
    first_t,
    second_t,
    up_t,
    heads,
    context,
    context_grad,
    residual,
    slope,
    hidden,
    send,
    recv,
    score,
    other,
    prob_low,
    score_low,
    flip,
    turned,
    gather_acc,
    log_sums,
    sums,
    up_sums,
    head_sums,
    small,
    small_x,
    small_y,
    small_z,
    gather_send,
    gather_recv,
    local_sem,
    scatter_send,
    scatter_recv,
    pair_send,
    pair_recv,
    row_send,
    row_recv,
    small_send,
    small_recv,
):
    place = lax.axis_index("fsdp")
    y = lax.axis_index("context")
    t = lax.axis_index("tensor")
    z = place // 2
    x = place % 2
    mine = x * 2 + y
    at_x = (1 - x) * 2 + y
    at_y = x * 2 + (1 - y)
    at_xy = (1 - x) * 2 + (1 - y)
    half = chain // 2
    to_x = {"fsdp": z * 2 + (1 - x)}
    to_y = {"context": 1 - y}
    to_t = {"tensor": 1 - t}

    def to_z(step):
        return {"fsdp": ((z + step) % chain) * 2 + x}

    def remote(source, target, send_sem, recv_sem, device):
        return pltpu.make_async_remote_copy(
            src_ref=source,
            dst_ref=target,
            send_sem=send_sem,
            recv_sem=recv_sem,
            device_id=device,
            device_id_type=MESH_ID,
        )

    slots = row_in.shape[0]
    own_slots = slots // 2
    quarter = own_slots // 2
    width = row_in.shape[1]

    barrier = pltpu.get_barrier_semaphore()
    for device in [to_x, to_y, to_t] + [to_z(step) for step in range(1, chain)]:
        pl.semaphore_signal(barrier, inc=1, device_id=device, device_id_type=MESH_ID)
    pl.semaphore_wait(barrier, chain + 2)

    shards = (
        [weight_in.at[:, k * COLS : (k + 1) * COLS] for k in range(3)]
        + [weight_out]
        + [weight_up.at[:, k * COLS : (k + 1) * COLS] for k in range(4)]
        + [weight_down.at[:, k * COLS : (k + 1) * COLS] for k in range(4)]
    )

    def slot_of(j):
        return j + 8 * (j // 8)

    def gather_copy(j, kind):
        buf = store.at[slot_of(j)]
        sems = (gather_send.at[j, kind], gather_recv.at[j, kind])
        if kind < 3:
            block = buf.at[z, mine]
            return remote(block, block, *sems, to_z(kind + 1))
        if kind == 3:
            return remote(buf.at[:, mine], buf.at[:, mine], *sems, to_x)
        if kind == 4:
            return remote(buf.at[:, mine], buf.at[:, mine], *sems, to_y)
        if kind == 5:
            return remote(buf.at[0:half, at_x], buf.at[0:half, at_x], *sems, to_y)
        return remote(buf.at[half:, at_y], buf.at[half:, at_y], *sems, to_x)

    for j in range(PIECES):
        pltpu.make_async_copy(shards[j], store.at[slot_of(j), z, mine], local_sem.at[j]).start()

    def load_done(j):
        pltpu.make_async_copy(shards[j], store.at[slot_of(j), z, mine], local_sem.at[j]).wait()

    def gather_z(j):
        for step in range(chain - 1):
            gather_copy(j, step).start()

    def gather_plane(j):
        for step in range(chain - 1):
            gather_copy(j, step).wait()
        gather_copy(j, 3).start()
        gather_copy(j, 4).start()

    def gather_corner(j):
        gather_copy(j, 3).wait()
        gather_copy(j, 5).start()
        gather_copy(j, 4).wait()
        gather_copy(j, 6).start()

    def gather_done(j):
        gather_copy(j, 5).wait()
        gather_copy(j, 6).wait()

    last = PIECES - 1
    last_buf = store.at[slot_of(last)]
    rows = weight_in.shape[0]

    def plane_first(kind):
        sems = (gather_send.at[last, kind], gather_recv.at[last, kind])
        if kind < 3:
            return remote(last_buf.at[z], last_buf.at[z], *sems, to_z(kind + 1))
        if kind == 3:
            return remote(last_buf.at[z, mine], last_buf.at[z, mine], *sems, to_x)
        if kind == 4:
            return remote(last_buf.at[z, mine], last_buf.at[z, mine], *sems, to_y)
        if kind == 5:
            block = last_buf.at[z, at_x, 0 : rows // 2]
            return remote(block, block, *sems, to_y)
        block = last_buf.at[z, at_y, rows // 2 :]
        return remote(block, block, *sems, to_x)

    def row_copies(source, target, which):
        mine_half = part(y, own_slots)
        local = pltpu.make_async_copy(source.at[y], target.at[mine_half], row_send.at[which, 2])
        place_there = pl.ds(pl.multiple_of(y * own_slots + t * quarter, quarter), quarter)
        across = remote(
            source.at[1 - y, part(t, quarter)],
            target.at[place_there],
            row_send.at[which, 0],
            row_recv.at[which, 0],
            to_y,
        )
        place_here = pl.ds(pl.multiple_of((1 - y) * own_slots + t * quarter, quarter), quarter)
        onward = remote(
            target.at[place_here], target.at[place_here], row_send.at[which, 1], row_recv.at[which, 1], to_t
        )
        return local, across, onward

    def row_back(source, target, which):
        mine_half = part(y, own_slots)
        local = pltpu.make_async_copy(source.at[mine_half], target.at[y], row_send.at[which, 2])
        from_here = pl.ds(pl.multiple_of((1 - y) * own_slots + t * quarter, quarter), quarter)
        across = remote(
            source.at[from_here],
            target.at[y, part(t, quarter)],
            row_send.at[which, 0],
            row_recv.at[which, 0],
            to_y,
        )
        block = target.at[1 - y, part(t, quarter)]
        onward = remote(block, block, row_send.at[which, 1], row_recv.at[which, 1], to_t)
        return local, across, onward

    token_local, token_across, token_on = row_copies(tokens, row_in, 0)
    up_local, up_across, up_on = row_copies(cotangent, row_up, 1)

    load_done(0)
    gather_z(0)
    token_local.start()
    token_across.start()
    load_done(last)
    plane_first(3).start()
    plane_first(4).start()
    for j in range(1, PIECES - 1):
        load_done(j)

    peak_out[...] = jnp.full(peak_out.shape, MASKED, F32)
    sums[...] = jnp.zeros(sums.shape, F32)

    def stats(values):
        average = jnp.mean(values, axis=1, keepdims=True)
        centered = values - average
        inverse = lax.rsqrt(jnp.mean(centered * centered, axis=1, keepdims=True) + EPSILON)
        return centered * inverse, inverse

    norm_rows = 32

    def norm_first(i):
        at = part(i, norm_rows)
        scaled, _ = stats(row_in[at, :].astype(F32))
        plain[at, :] = (scaled * first_gain[...] + first_shift[...]).astype(BF)

    def turn(source, target):
        def body(j):
            target[part(j, 128), :] = source[:, part(j, 128)].T

        loop(width // 128, body)

    token_across.wait()
    token_on.start()
    token_local.wait()
    gather_plane(0)
    gather_z(1)
    plane_first(3).wait()
    plane_first(5).start()
    plane_first(4).wait()
    plane_first(6).start()
    token_on.wait()
    loop(slots // norm_rows, norm_first)
    gather_plane(1)
    gather_z(2)
    gather_corner(0)
    up_local.start()
    up_across.start()
    turn(plain, first_t)

    def tick(j):
        gather_plane(j)
        gather_z(j + 1)
        gather_corner(j - 1)
        gather_done(j - 2)

    def project(c, which):
        at = part(c, TILE)
        tile = store[which, :, :, :, at].reshape(width, TILE)
        heads[which, c] = (nn(plain[...], tile) + bias_three[which, :, at]).astype(BF)

    def project_step(j):
        tick(j)
        loop(2, lambda c: project(c, j - 2))

    loop(5, project_step, 2)
    up_across.wait()
    up_on.start()
    up_local.wait()

    lane = lax.broadcasted_iota(jnp.int32, (slots, 128), 1)
    chunk = 64
    n_chunks = slots // chunk

    def head_operands(pair, h):
        where_pair = part(pair % 2, 128)
        query = heads[0, pair // 2, :, where_pair].astype(F32) * (HEAD_DIM**-0.5)
        key = heads[1, pair // 2, :, where_pair].astype(F32)
        own = (lane < HEAD_DIM) if h == 0 else (lane >= HEAD_DIM)
        first = HEAD_DIM if h == 0 else 0
        flag = keep_col[...]
        query = jnp.where(own, query, jnp.where(lane == first, flag, jnp.where(lane == first + 1, 1.0 - flag, 0.0)))
        key = jnp.where(
            lane == first, -BIG * (1.0 - flag), jnp.where(lane == first + 1, -BIG * flag, key)
        )
        return query.astype(BF), key.astype(BF), own

    def attend(pair):
        where_pair = part(pair % 2, 128)
        turned[...] = heads[2, pair // 2, :, where_pair].T
        for h in range(2):
            query, key, _ = head_operands(pair, h)
            score[...] = nt(key, query)

            def top(i, best):
                return jnp.maximum(best, jnp.max(score[part(i, chunk), :].reshape(-1, 8, slots), axis=0))

            best = lax.fori_loop(0, n_chunks, top, jnp.full((8, slots), -3e38, F32))
            highest = jnp.max(best, axis=0, keepdims=True)

            def power(i, total):
                at = part(i, chunk)
                powers = jnp.exp(score[at, :] - highest)
                prob_low[at, :] = powers.astype(BF)
                return total + fold(powers)

            total = lax.fori_loop(0, n_chunks, power, jnp.zeros((8, slots), F32))
            total = jnp.sum(total, axis=0, keepdims=True)
            mixed = nn(turned[h * HEAD_DIM : (h + 1) * HEAD_DIM, :], prob_low[...])
            flip[h * HEAD_DIM : (h + 1) * HEAD_DIM, :] = mixed / total
            log_sums[2 * pair + h] = highest + jnp.log(total)
            summit = jnp.max(jnp.where(keep_row[...] > 0.0, highest, MASKED), axis=1, keepdims=True)
            spots = lax.broadcasted_iota(jnp.int32, peak_out.shape, 1)
            peak_out[...] = jnp.where(spots == 2 * pair + h, summit, peak_out[...])
        context[pair // 2, :, where_pair] = flip[...].T.astype(BF)

    def attend_step(i):
        tick(5 + i)
        attend(i)

    loop(4, attend_step)

    def mask_rows(i):
        at = part(i, 64)
        row_up[at, :] = (row_up[at, :].astype(F32) * keep_col[at, :]).astype(BF)

    up_on.wait()
    loop(slots // 64, mask_rows)
    turn(row_up, up_t)

    def pair_copy(slot, j):
        return remote(send.at[j], recv.at[slot, j], pair_send.at[j], pair_recv.at[slot, j], to_t)

    def pair_sum(slot, product):
        def body(j):
            send[j] = product(j).astype(BF)
            pair_copy(slot, j).start()

        loop(4, body)
        for j in range(4):
            pair_copy(slot, j).wait()

    def summed(slot, at):
        return jnp.concatenate(
            [send[j, at, :].astype(F32) + recv[slot, j, at, :].astype(F32) for j in range(4)], axis=1
        )

    def weight_rows(piece, j, c):
        return store[piece, j, :, :, c * TILE : (c + 1) * TILE].reshape(TILE, TILE)

    def attended(j):
        return nt(context[0], weight_rows(3, j, 0)) + nt(context[1], weight_rows(3, j, 1))

    tick(9)
    pair_sum(0, attended)

    def norm_second(i):
        at = part(i, norm_rows)
        values = row_in[at, :].astype(F32) + summed(0, at) + output_bias[0:1, :]
        residual[at, :] = values
        scaled, _ = stats(values)
        plain[at, :] = (scaled * second_gain[...] + second_shift[...]).astype(BF)

    loop(slots // norm_rows, norm_second)

    gather_plane(10)
    for kind in (5, 6):
        plane_first(kind).wait()
    for kind in range(chain - 1):
        plane_first(kind).start()
    gather_corner(9)
    gather_done(8)

    def activate(c):
        at = part(c % 2, TILE)
        tile = store[4 + c // 2, :, :, :, at].reshape(width, TILE)
        score[:, 0:TILE] = nn(plain[...], tile) + up_bias[c]

        def rows_of(i):
            spot = part(i, 64)
            pre = score[spot, 0:TILE]
            chance = 0.5 * (1.0 + lax.erf(pre * HALF_ROOT))
            hidden[c, spot, :] = (pre * chance).astype(BF)
            slope[c, spot, :] = (chance + pre * jnp.exp(-0.5 * pre * pre) * DENSITY).astype(BF)

        loop(slots // 64, rows_of)

    loop(4, activate)
    gather_corner(10)
    gather_done(9)
    loop(8, activate, 4)
    turn(plain, second_t)

    def scatter_copy(p, kind):
        buf = store.at[8 + p]
        sems = (scatter_send.at[p, kind], scatter_recv.at[p, kind])
        if kind == 0:
            return remote(buf.at[0:half, at_xy], near.at[p, 0], *sems, to_y)
        if kind == 1:
            return remote(buf.at[half:, at_xy], near.at[p, 1], *sems, to_x)
        if kind == 2:
            return remote(buf.at[:, at_x], mid.at[p, 0], *sems, to_x)
        if kind == 3:
            return remote(buf.at[:, at_y], mid.at[p, 1], *sems, to_y)
        step = kind - 3
        return remote(buf.at[(z + step) % chain, mine], far.at[p, step - 1], *sems, to_z(step))

    def scatter_corner(p):
        scatter_copy(p, 0).start()
        scatter_copy(p, 1).start()

    def added(left, right):
        return (left.astype(F32) + right.astype(F32)).astype(BF)

    def scatter_plane(p):
        scatter_copy(p, 0).wait()
        for k in range(half):
            store[8 + p, k, at_x] = added(store[8 + p, k, at_x], near[p, 0, k])
        scatter_copy(p, 1).wait()
        for k in range(half):
            store[8 + p, half + k, at_y] = added(store[8 + p, half + k, at_y], near[p, 1, k])
        scatter_copy(p, 2).start()
        scatter_copy(p, 3).start()

    def scatter_z(p):
        scatter_copy(p, 2).wait()
        scatter_copy(p, 3).wait()
        for k in range(chain):
            store[8 + p, k, mine] = (
                store[8 + p, k, mine].astype(F32) + mid[p, 0, k].astype(F32) + mid[p, 1, k].astype(F32)
            ).astype(BF)
        for step in range(1, chain):
            scatter_copy(p, 3 + step).start()

    def scatter_done(p, target, at):
        for step in range(1, chain):
            scatter_copy(p, 3 + step).wait()
        total = store[8 + p, z, mine].astype(F32)
        for step in range(1, chain):
            total = total + far[p, step - 1].astype(F32)
        target[:, at] = total

    def finish(p):
        if p < 4:
            scatter_done(p, down_sum, slice(p * COLS, (p + 1) * COLS))
        elif p < 8:
            scatter_done(p, up_sum, slice((p - 4) * COLS, (p - 3) * COLS))
        elif p == 8:
            scatter_done(p, out_sum, slice(0, COLS))
        else:
            scatter_done(p, in_sum, slice((p - 9) * COLS, (p - 8) * COLS))

    def scatter_tick(k):
        if k < PIECES:
            scatter_plane(k)
        if 0 <= k - 1 < PIECES:
            scatter_z(k - 1)
        if 0 <= k - 2 < PIECES:
            finish(k - 2)

    def gradient(left, right, piece, c):
        def body(m):
            block = nn(left[part(m, width // 2), :], right)
            store[8 + piece, part(m, half), :, :, part(c, TILE)] = block.astype(BF).reshape(half, 4, rows, TILE)

        loop(2, body)

    def down_piece(p):
        loop(2, lambda c: gradient(up_t, hidden[2 * p + c], p, c))
        scatter_corner(p)

    loop(4, down_piece)
    gather_done(10)
    for kind in range(chain - 1):
        plane_first(kind).wait()

    def back_hidden(c):
        at = part(c % 2, TILE)
        tile = store[16 + c // 2, :, :, :, at].reshape(width, TILE)
        score[:, 0:TILE] = nn(row_up[...], tile)

        def rows_of(i, total):
            spot = part(i, 64)
            grad = (score[spot, 0:TILE] * slope[c, spot, :].astype(F32)).astype(BF)
            slope[c, spot, :] = grad
            return total + fold(grad.astype(F32))

        total = lax.fori_loop(0, slots // 64, rows_of, jnp.zeros((8, TILE), F32))
        up_sums[c] = jnp.sum(total, axis=0, keepdims=True)

    loop(8, back_hidden)
    scatter_tick(0)

    def up_piece(p):
        loop(2, lambda c: gradient(second_t, slope[2 * p + c], 4 + p, c))
        scatter_corner(4 + p)

    loop(2, up_piece)
    scatter_tick(1)
    loop(4, up_piece, 2)
    scatter_tick(2)

    def mixed(j):
        total = nt(hidden[0], weight_rows(16, j, 0))
        for c in range(1, 8):
            total = total + nt(hidden[c], weight_rows(16 + c // 2, j, c % 2))
        return total

    pair_sum(1, mixed)

    def output_rows(i):
        at = part(i, norm_rows)
        values = residual[at, :] + summed(1, at) + output_bias[1:2, :]
        plain[at, :] = (values * keep_col[at, :]).astype(BF)

    loop(slots // norm_rows, output_rows)
    block_local, block_across, block_on = row_back(plain, block_out, 2)
    block_local.start()
    block_across.start()
    scatter_tick(3)

    def second_back(j):
        total = nt(slope[0], weight_rows(4, j, 0))
        for c in range(1, 8):
            total = total + nt(slope[c], weight_rows(4 + c // 2, j, c % 2))
        return total

    pair_sum(0, second_back)

    def norm_second_back(i):
        at = part(i, norm_rows)
        scaled, inverse = stats(residual[at, :])
        incoming = summed(0, at)
        weighted = incoming * second_gain[...]
        upstream = row_up[at, :].astype(F32)
        bracket = (
            weighted
            - jnp.mean(weighted, axis=1, keepdims=True)
            - scaled * jnp.mean(weighted * scaled, axis=1, keepdims=True)
        )
        total = upstream + inverse * bracket
        residual[at, :] = total
        low = total.astype(BF)
        for j in range(4):
            hidden[4 + j, at, :] = low[:, j * TILE : (j + 1) * TILE]
        sums[0] += fold(incoming * scaled)
        sums[1] += fold(incoming)
        sums[2] += fold(total)
        sums[3] += fold(upstream)

    loop(slots // norm_rows, norm_second_back)
    for j in range(4):
        for k in range(2):
            at = j * TILE + k * 128
            up_t[at : at + 128, :] = hidden[4 + j, :, k * 128 : (k + 1) * 128].T
    scatter_tick(4)
    loop(2, lambda c: gradient(up_t, context[c], 8, c))
    scatter_corner(8)

    def back_context(c):
        total = None
        for j in range(4):
            tile = store[3, j, :, :, part(c, TILE)].reshape(TILE, TILE)
            term = nn(hidden[4 + j], tile)
            total = term if total is None else total + term
        context_grad[c] = total.astype(BF)

    loop(2, back_context)
    block_across.wait()
    block_on.start()

    def attend_back(pair):
        where_pair = part(pair % 2, 128)
        turned[...] = heads[1, pair // 2, :, where_pair].T
        value = heads[2, pair // 2, :, where_pair]
        incoming = context_grad[pair // 2, :, where_pair]
        for h in range(2):
            query, key, own = head_operands(pair, h)
            own_in = jnp.where(own, incoming.astype(F32), 0.0).astype(BF)
            score[...] = nt(key, query)
            other[...] = nt(value, own_in)
            logs = log_sums[2 * pair + h]

            def power(i, total):
                at = part(i, chunk)
                probs = jnp.exp(score[at, :] - logs)
                score[at, :] = probs
                prob_low[at, :] = probs.astype(BF)
                return total + fold(probs * other[at, :])

            total = lax.fori_loop(0, n_chunks, power, jnp.zeros((8, slots), F32))
            centre = jnp.sum(total, axis=0, keepdims=True)

            def rest(i):
                at = part(i, chunk)
                score_low[at, :] = (score[at, :] * (other[at, :] - centre)).astype(BF)

            loop(n_chunks, rest)
            value_grad = nn(prob_low[...], own_in)
            key_grad = nn(score_low[...], query)
            if h == 0:
                gather_acc[0] = value_grad
                gather_acc[1] = key_grad
            else:
                gather_acc[0] += value_grad
                gather_acc[1] = jnp.where(own, key_grad, gather_acc[1])
            flip[h * HEAD_DIM : (h + 1) * HEAD_DIM, :] = nn(
                turned[h * HEAD_DIM : (h + 1) * HEAD_DIM, :], score_low[...]
            ) * (HEAD_DIM**-0.5)
        query_low = flip[...].T.astype(BF)
        value_low = gather_acc[0].astype(BF)
        heads[0, pair // 2, :, where_pair] = query_low
        heads[1, pair // 2, :, where_pair] = gather_acc[1].astype(BF)
        heads[2, pair // 2, :, where_pair] = value_low
        head_sums[0, pair] = jnp.sum(query_low.astype(F32), axis=0, keepdims=True)
        head_sums[1, pair] = jnp.sum(value_low.astype(F32), axis=0, keepdims=True)

    for pair in range(4):
        attend_back(pair)
        scatter_tick(5 + pair)

    def in_piece(i):
        loop(2, lambda c: gradient(first_t, heads[i, c], 9 + i, c))
        scatter_corner(9 + i)

    loop(3, in_piece)

    def first_back(j):
        total = None
        for i in range(3):
            for c in range(2):
                term = nt(heads[i, c], weight_rows(i, j, c))
                total = term if total is None else total + term
        return total

    pair_sum(1, first_back)
    scatter_tick(9)

    def norm_first_back(i):
        at = part(i, norm_rows)
        scaled, inverse = stats(row_in[at, :].astype(F32))
        incoming = summed(1, at)
        weighted = incoming * first_gain[...]
        bracket = (
            weighted
            - jnp.mean(weighted, axis=1, keepdims=True)
            - scaled * jnp.mean(weighted * scaled, axis=1, keepdims=True)
        )
        row_in[at, :] = (residual[at, :] + inverse * bracket).astype(BF)
        sums[4] += fold(incoming * scaled)
        sums[5] += fold(incoming)

    loop(slots // norm_rows, norm_first_back)
    grad_local, grad_across, grad_on = row_back(row_in, token_grad, 3)
    grad_local.start()
    grad_across.start()

    def collapse(k):
        return jnp.sum(sums[k], axis=0, keepdims=True)

    small[0:1, :] = collapse(4)
    small[1:2, :] = collapse(5)
    small[2:3, :] = jnp.concatenate([head_sums[i, k] for i in range(2) for k in range(4)], axis=1)
    small[3:4, :] = collapse(2)
    small[4:5, :] = collapse(3)
    small[5:6, :] = collapse(0)
    small[6:7, :] = collapse(1)
    small[7:8, :] = jnp.concatenate([up_sums[k] for k in range(4)], axis=1)
    small[8:9, :] = jnp.concatenate([up_sums[4 + k] for k in range(4)], axis=1)
    small[9:10, :] = jnp.concatenate([peak_out[0:1, :]] * 8, axis=1)
    small[10:16, :] = jnp.zeros((6, small.shape[1]), F32)
    row_index = lax.broadcasted_iota(jnp.int32, small.shape, 0)

    def joined(left, right):
        return jnp.where(row_index == 9, jnp.maximum(left, right), left + right)

    def small_copy(source, target, k, device):
        return remote(source, target, small_send.at[k], small_recv.at[k], device)

    over_x = small_copy(small, small_x.at[0], 0, to_x)
    over_x.start()
    scatter_tick(10)
    over_x.wait()
    small_x[1] = joined(small[...], small_x[0])
    over_y = small_copy(small_x.at[1], small_y, 1, to_y)
    over_y.start()
    grad_across.wait()
    grad_on.start()
    scatter_tick(11)
    over_y.wait()
    small_z[z] = joined(small_x[1], small_y[...])
    over_z = [small_copy(small_z.at[z], small_z.at[z], 1 + step, to_z(step)) for step in range(1, chain)]
    for copy in over_z:
        copy.start()
    scatter_tick(12)
    for copy in over_z:
        copy.wait()
    total = small_z[0]
    for k in range(1, chain):
        total = joined(total, small_z[k])
    small_out[...] = total
    scatter_tick(13)
    block_local.wait()
    block_on.wait()
    grad_local.wait()
    grad_on.wait()


def on_device_fused(
    tokens,
    segments,
    first_gain,
    first_shift,
    input_weight,
    input_bias,
    output_weight,
    output_bias,
    second_gain,
    second_shift,
    up_weight,
    up_bias,
    down_weight,
    cotangent,
    chain,
):
    group, tok_rows, width = tokens.shape
    slots = segments.shape[1]
    rows = input_weight.shape[0]
    flags = lax.dynamic_slice_in_dim(segments, lax.axis_index("context"), 1, 0).astype(F32)
    bias_three = jnp.stack([input_bias[0], jnp.zeros_like(input_bias[0]), input_bias[1]])[:, None, :]
    operands = (
        tokens,
        cotangent,
        input_weight.reshape(rows, -1),
        output_weight,
        up_weight,
        down_weight,
        first_gain[None],
        first_shift[None],
        bias_three,
        output_bias,
        second_gain[None],
        second_shift[None],
        up_bias.reshape(8, 1, TILE),
        flags.reshape(slots, 1),
        flags,
    )
    anywhere = pl.BlockSpec(memory_space=pl.ANY)
    vmem = pl.BlockSpec(memory_space=pltpu.VMEM)
    half = chain // 2
    block = (rows, COLS)
    dma = pltpu.SemaphoreType.DMA
    results = pl.pallas_call(
        functools.partial(layer_kernel, chain),
        out_shape=(
            jax.ShapeDtypeStruct(tokens.shape, BF),
            jax.ShapeDtypeStruct(tokens.shape, BF),
            jax.ShapeDtypeStruct((rows, 3 * COLS), F32),
            jax.ShapeDtypeStruct((rows, COLS), F32),
            jax.ShapeDtypeStruct((rows, 4 * COLS), F32),
            jax.ShapeDtypeStruct((rows, 4 * COLS), F32),
            jax.ShapeDtypeStruct((16, width), F32),
            jax.ShapeDtypeStruct((8, 128), F32),
        ),
        in_specs=[anywhere] * 6 + [vmem] * 9,
        out_specs=[anywhere] * 2 + [vmem] * 6,
        scratch_shapes=[
            pltpu.VMEM((20, chain, 4) + block, BF),
            pltpu.VMEM((PIECES, 2, half) + block, BF),
            pltpu.VMEM((PIECES, 2, chain) + block, BF),
            pltpu.VMEM((PIECES, chain - 1) + block, BF),
            pltpu.VMEM((slots, width), BF),
            pltpu.VMEM((slots, width), BF),
            pltpu.VMEM((slots, width), BF),
            pltpu.VMEM((width, slots), BF),
            pltpu.VMEM((width, slots), BF),
            pltpu.VMEM((width, slots), BF),
            pltpu.VMEM((3, 2, slots, TILE), BF),
            pltpu.VMEM((2, slots, TILE), BF),
            pltpu.VMEM((2, slots, TILE), BF),
            pltpu.VMEM((slots, width), F32),
            pltpu.VMEM((8, slots, TILE), BF),
            pltpu.VMEM((8, slots, TILE), BF),
            pltpu.VMEM((4, slots, TILE), BF),
            pltpu.VMEM((2, 4, slots, TILE), BF),
            pltpu.VMEM((slots, slots), F32),
            pltpu.VMEM((slots, slots), F32),
            pltpu.VMEM((slots, slots), BF),
            pltpu.VMEM((slots, slots), BF),
            pltpu.VMEM((128, slots), F32),
            pltpu.VMEM((128, slots), BF),
            pltpu.VMEM((2, slots, 128), F32),
            pltpu.VMEM((8, 1, slots), F32),
            pltpu.VMEM((6, 8, width), F32),
            pltpu.VMEM((8, 1, TILE), F32),
            pltpu.VMEM((2, 4, 1, 128), F32),
            pltpu.VMEM((16, width), F32),
            pltpu.VMEM((2, 16, width), F32),
            pltpu.VMEM((16, width), F32),
            pltpu.VMEM((chain, 16, width), F32),
            dma((PIECES, 7)),
            dma((PIECES, 7)),
            dma((PIECES,)),
            dma((PIECES, 7)),
            dma((PIECES, 7)),
            dma((4,)),
            dma((2, 4)),
            dma((4, 3)),
            dma((4, 2)),
            dma((2 + chain,)),
            dma((2 + chain,)),
        ],
        compiler_params=pltpu.CompilerParams(
            collective_id=0, has_side_effects=True, vmem_limit_bytes=67043328
        ),
        name="layer",
    )(*operands)
    block_output, tokens_gradient, in_sum, out_sum, up_sum, down_sum, small, _ = results
    count = input_weight.shape[2] // HEAD_DIM
    factor = CLIP_LIMIT / jnp.maximum(small[9, :count], CLIP_LIMIT)
    column_scale = jnp.repeat(jnp.sqrt(factor), HEAD_DIM)
    clipped_weight = input_weight[:, :2, :].astype(F32) * column_scale[None, None, :]
    local_width = input_weight.shape[2]
    return (
        block_output,
        tokens_gradient.astype(F32),
        small[0],
        small[1],
        in_sum.reshape(rows, 3, local_width),
        small[2].reshape(2, local_width),
        out_sum,
        small[3:5],
        small[5],
        small[6],
        up_sum,
        small[7:9].reshape(-1),
        down_sum,
        clipped_weight,
        factor,
    )


def on_device(
    tokens,
    segments,
    first_gain,
    first_shift,
    input_weight,
    input_bias,
    output_weight,
    output_bias,
    second_gain,
    second_shift,
    up_weight,
    up_bias,
    down_weight,
    cotangent,
):
    group = tokens.shape[0]
    tok_rows = tokens.shape[1]
    width = tokens.shape[2]
    score_scale = HEAD_DIM ** (-0.5)
    position = lax.axis_index("context") * tok_rows
    query_segments = lax.dynamic_slice_in_dim(segments, position, tok_rows, 1)
    allowed = segments[:, None, :] == query_segments[:, :, None]
    real_pairs = allowed & (query_segments[:, :, None] > 0)
    keep_rows = (query_segments > 0).astype(jnp.float32).reshape(-1)[:, None]
    input_full, output_full = (
        lax.all_gather(input_weight, ("fsdp", "context"), axis=0, tiled=True),
        lax.all_gather(output_weight, ("fsdp", "context"), axis=0, tiled=True),
    )
    tokens_float = tokens.astype(jnp.float32).reshape(group * tok_rows, width)
    normed_one, scaled_one, inverse_one = normalize(tokens_float, first_gain, first_shift)
    first_operand = normed_one.astype(jnp.bfloat16)
    projected = jnp.einsum(
        "td,dcf->tcf", first_operand, input_full, preferred_element_type=jnp.float32
    )
    bias_rows = jnp.stack([input_bias[0], jnp.zeros_like(input_bias[0]), input_bias[1]])
    projected = (projected + bias_rows[None]).astype(jnp.bfloat16)
    local_width = projected.shape[2]
    projected = projected.reshape(group, tok_rows, 3, local_width)
    sources = lax.all_gather(projected[:, :, 1:], "context", axis=1, tiled=True)
    query_heads = split_heads(projected[:, :, 0])
    key_heads = split_heads(sources[:, :, 0])
    value_heads = split_heads(sources[:, :, 1])

    def head_forward(operands):
        query_one, key_one, value_one = operands
        logits = (
            jnp.einsum("gqd,gkd->gqk", query_one, key_one, preferred_element_type=jnp.float32)
            * score_scale
        )
        masked = jnp.where(allowed, logits, MASKED)
        summit = jnp.max(jnp.where(real_pairs, logits, MASKED))
        highest = jnp.max(masked, axis=2, keepdims=True)
        powers = jnp.exp(masked - highest)
        totals = jnp.sum(powers, axis=2, keepdims=True)
        weights_low = (powers / totals).astype(jnp.bfloat16)
        mixed = jnp.einsum(
            "gqk,gkd->gqd", weights_low, value_one, preferred_element_type=jnp.float32
        )
        return (mixed.astype(jnp.bfloat16), (highest + jnp.log(totals))[:, :, 0], summit)

    head_context, log_totals, summits = lax.map(head_forward, (query_heads, key_heads, value_heads))
    context = join_heads(head_context).reshape(group * tok_rows, local_width)
    attended = lax.psum(
        jnp.einsum("tf,df->td", context, output_full, preferred_element_type=jnp.float32), "tensor"
    )
    residual = tokens_float + attended + output_bias[0]
    peaks = lax.pmax(summits, ("fsdp", "context"))
    up_full, down_full = (
        lax.all_gather(up_weight, ("fsdp", "context"), axis=0, tiled=True),
        lax.all_gather(down_weight, ("fsdp", "context"), axis=0, tiled=True),
    )
    normed_two, scaled_two, inverse_two = normalize(residual, second_gain, second_shift)
    second_operand = normed_two.astype(jnp.bfloat16)
    pre_act = jnp.dot(second_operand, up_full, preferred_element_type=jnp.float32) + up_bias
    hidden = jax.nn.gelu(pre_act, approximate=False).astype(jnp.bfloat16)
    mixed_sum = lax.psum(
        jnp.einsum("tf,df->td", hidden, down_full, preferred_element_type=jnp.float32).astype(
            jnp.bfloat16
        ),
        "tensor",
    ).astype(jnp.float32)
    block_output = ((residual + mixed_sum + output_bias[1]) * keep_rows).astype(jnp.bfloat16)
    factor = CLIP_LIMIT / jnp.maximum(peaks, CLIP_LIMIT)
    column_scale = jnp.repeat(jnp.sqrt(factor), HEAD_DIM)
    clipped_weight = input_weight[:, :2, :].astype(jnp.float32) * column_scale[None, None, :]
    input_full, output_full, up_full, down_full = (
        lax.all_gather(input_weight, ("fsdp", "context"), axis=0, tiled=True),
        lax.all_gather(output_weight, ("fsdp", "context"), axis=0, tiled=True),
        lax.all_gather(up_weight, ("fsdp", "context"), axis=0, tiled=True),
        lax.all_gather(down_weight, ("fsdp", "context"), axis=0, tiled=True),
    )
    upstream = cotangent.astype(jnp.float32).reshape(group * tok_rows, width) * keep_rows
    upstream_low = upstream.astype(jnp.bfloat16)
    down_gradient = jnp.einsum(
        "td,tf->df", upstream_low, hidden, preferred_element_type=jnp.float32
    )
    pre_gradient = (
        jnp.dot(upstream_low, down_full, preferred_element_type=jnp.float32) * gelu_slope(pre_act)
    ).astype(jnp.bfloat16)
    up_gradient = jnp.einsum(
        "td,tf->df", second_operand, pre_gradient, preferred_element_type=jnp.float32
    )
    up_bias_gradient = jnp.sum(pre_gradient.astype(jnp.float32), axis=0)
    second_gradient = lax.psum(
        jnp.einsum("tf,df->td", pre_gradient, up_full, preferred_element_type=jnp.float32), "tensor"
    )
    through_two, second_gain_gradient, second_shift_gradient = normalize_back(
        second_gradient, scaled_two, inverse_two, second_gain
    )
    residual_gradient = upstream + through_two
    output_bias_gradient = jnp.stack(
        [jnp.sum(residual_gradient, axis=0), jnp.sum(upstream, axis=0)]
    )
    attend_low = residual_gradient.astype(jnp.bfloat16)
    output_gradient = jnp.einsum(
        "td,tf->df", attend_low, context, preferred_element_type=jnp.float32
    )
    context_back = jnp.dot(attend_low, output_full, preferred_element_type=jnp.float32).astype(
        jnp.bfloat16
    )
    context_gradient = split_heads(context_back.reshape(group, tok_rows, local_width))

    def head_backward(operands):
        query_one, key_one, value_one, incoming, log_total = operands
        logits = (
            jnp.einsum("gqd,gkd->gqk", query_one, key_one, preferred_element_type=jnp.float32)
            * score_scale
        )
        probs = jnp.exp(jnp.where(allowed, logits, MASKED) - log_total[:, :, None])
        prob_gradient = jnp.einsum(
            "gqd,gkd->gqk", incoming, value_one, preferred_element_type=jnp.float32
        )
        centre = jnp.sum(probs * prob_gradient, axis=2, keepdims=True)
        score_low = (probs * (prob_gradient - centre) * score_scale).astype(jnp.bfloat16)
        query_gradient = jnp.einsum(
            "gqk,gkd->gqd", score_low, key_one, preferred_element_type=jnp.float32
        ).astype(jnp.bfloat16)
        key_gradient = jnp.einsum(
            "gqk,gqd->gkd", score_low, query_one, preferred_element_type=jnp.float32
        )
        value_gradient = jnp.einsum(
            "gqk,gqd->gkd", probs.astype(jnp.bfloat16), incoming, preferred_element_type=jnp.float32
        )
        return (query_gradient, key_gradient, value_gradient)

    query_grads, key_grads, value_grads = lax.map(
        head_backward, (query_heads, key_heads, value_heads, context_gradient, log_totals)
    )
    source_terms = jnp.stack([join_heads(key_grads), join_heads(value_grads)], axis=2)
    source_sums = lax.psum_scatter(
        source_terms.astype(jnp.bfloat16), "context", scatter_dimension=1, tiled=True
    )
    source_low = source_sums.reshape(group * tok_rows, 2, local_width)
    query_flat = join_heads(query_grads).reshape(group * tok_rows, local_width)
    projected_gradient = jnp.concatenate([query_flat[:, None, :], source_low], axis=1)
    input_gradient = jnp.einsum(
        "td,tcf->dcf", first_operand, projected_gradient, preferred_element_type=jnp.float32
    )
    input_bias_gradient = jnp.stack(
        [
            jnp.sum(projected_gradient[:, 0].astype(jnp.float32), axis=0),
            jnp.sum(projected_gradient[:, 2].astype(jnp.float32), axis=0),
        ]
    )
    first_gradient = lax.psum(
        jnp.einsum(
            "tcf,dcf->td", projected_gradient, input_full, preferred_element_type=jnp.float32
        ).astype(jnp.bfloat16),
        "tensor",
    ).astype(jnp.float32)
    through_one, first_gain_gradient, first_shift_gradient = normalize_back(
        first_gradient, scaled_one, inverse_one, first_gain
    )
    tokens_gradient = (residual_gradient + through_one).reshape(group, tok_rows, width)
    block_output = block_output.reshape(group, tok_rows, width)
    (
        first_gain_sum,
        first_shift_sum,
        input_bias_sum,
        output_bias_sum,
        second_gain_sum,
        second_shift_sum,
        up_bias_sum,
    ) = lax.psum(
        (
            first_gain_gradient,
            first_shift_gradient,
            input_bias_gradient,
            output_bias_gradient,
            second_gain_gradient,
            second_shift_gradient,
            up_bias_gradient,
        ),
        ("fsdp", "context"),
    )
    input_sum, output_sum, up_sum, down_sum = (
        lax.psum_scatter(input_gradient, ("fsdp", "context"), scatter_dimension=0, tiled=True),
        lax.psum_scatter(output_gradient, ("fsdp", "context"), scatter_dimension=0, tiled=True),
        lax.psum_scatter(up_gradient, ("fsdp", "context"), scatter_dimension=0, tiled=True),
        lax.psum_scatter(down_gradient, ("fsdp", "context"), scatter_dimension=0, tiled=True),
    )
    return (
        block_output,
        tokens_gradient,
        first_gain_sum,
        first_shift_sum,
        input_sum,
        input_bias_sum,
        output_sum,
        output_bias_sum,
        second_gain_sum,
        second_shift_sum,
        up_sum,
        up_bias_sum,
        down_sum,
        clipped_weight,
        factor,
    )


def solution(mesh):
    placed = (
        P("fsdp", "context", None),
        P("fsdp", None),
        P(),
        P(),
        P(("fsdp", "context"), None, "tensor"),
        P(None, "tensor"),
        P(("fsdp", "context"), "tensor"),
        P(),
        P(),
        P(),
        P(("fsdp", "context"), "tensor"),
        P("tensor"),
        P(("fsdp", "context"), "tensor"),
        P("fsdp", "context", None),
    )
    chain = mesh.shape["fsdp"] // 2
    step = on_device
    if mesh.shape["context"] == 2 and mesh.shape["tensor"] == 2 and chain == 4:
        step = functools.partial(on_device_fused, chain=chain)
    return jax.shard_map(
        step,
        mesh=mesh,
        in_specs=placed,
        out_specs=(
            P("fsdp", "context", None),
            P("fsdp", "context", None),
            P(),
            P(),
            P(("fsdp", "context"), None, "tensor"),
            P(None, "tensor"),
            P(("fsdp", "context"), "tensor"),
            P(),
            P(),
            P(),
            P(("fsdp", "context"), "tensor"),
            P("tensor"),
            P(("fsdp", "context"), "tensor"),
            P(("fsdp", "context"), None, "tensor"),
            P("tensor"),
        ),
        check_vma=False,
    )
```

```python
import functools

import jax
import jax.numpy as jnp
from jax import lax
from jax.experimental import pallas as pl
from jax.experimental.pallas import tpu as pltpu
from jax.sharding import PartitionSpec as P

HEAD_DIM = 64


EPSILON = 1e-06
CLIP_LIMIT = 1.5
MASKED = -1e30
HALF_ROOT = 0.7071067811865476
DENSITY = 0.3989422804014327


def normalize(values, gain, shift):
    average = jnp.mean(values, axis=-1, keepdims=True)
    centered = values - average
    inverse = lax.rsqrt(jnp.mean(centered * centered, axis=-1, keepdims=True) + EPSILON)
    scaled = centered * inverse
    return (scaled * gain + shift, scaled, inverse)


def normalize_back(incoming, scaled, inverse, gain):
    weighted = incoming * gain
    bracket = (
        weighted
        - jnp.mean(weighted, axis=-1, keepdims=True)
        - scaled * jnp.mean(weighted * scaled, axis=-1, keepdims=True)
    )
    return (inverse * bracket, jnp.sum(incoming * scaled, axis=0), jnp.sum(incoming, axis=0))


def gelu_slope(values):
    return (
        0.5 * (1.0 + lax.erf(values * HALF_ROOT))
        + values * jnp.exp(-0.5 * values * values) * DENSITY
    )


def split_heads(values):
    shaped = values.reshape(values.shape[0], values.shape[1], -1, HEAD_DIM)
    return jnp.transpose(shaped, (2, 0, 1, 3))


def join_heads(values):
    moved = jnp.transpose(values, (1, 2, 0, 3))
    return moved.reshape(moved.shape[0], moved.shape[1], -1)


BF = jnp.bfloat16
F32 = jnp.float32
COLS = 512
TILE = 256
PIECES = 12
BIG = 1e30
MESH_ID = pl.DeviceIdType.MESH
GATHER_PIECES = (
    (0, 0, 256),
    (0, 256, 256),
    (1, 0, 512),
    (2, 0, 512),
    (3, 0, 512),
    (4, 0, 512),
    (5, 0, 512),
    (6, 0, 512),
    (7, 0, 512),
    (8, 0, 512),
    (9, 0, 512),
    (10, 0, 512),
    (11, 0, 512),
)
SCATTER_PIECES = (
    (0, 0, 512),
    (1, 0, 512),
    (2, 0, 512),
    (3, 0, 512),
    (4, 0, 512),
    (5, 0, 512),
    (6, 0, 512),
    (7, 0, 512),
    (8, 0, 512),
    (9, 0, 512),
    (10, 0, 256),
    (10, 256, 256),
    (11, 0, 256),
    (11, 256, 256),
)
GATHER_KINDS = (0, 1, 0, 0, 1, 1, 0, 0, 1, 0, 0, 1, 1)
SCATTER_KINDS = (1, 1, 1, 0, 1, 1, 0, 1, 1, 0, 0, 0, 0, 0)
GATHER_SWAPPED = (0, 0, 0, 1, 0, 0, 0, 0, 0, 0, 0, 0, 0)
SCATTER_SWAPPED = (0, 0, 0, 0, 0, 0, 1, 0, 0, 0, 1, 0, 0, 0)
GATHER, SCATTER, ROWS, SMALL, COMPUTE = range(5)
TOKENS, COTANGENT, BLOCK, GRADIENT = range(4)
(
    NORM_ONE,
    TURN_ONE,
    PROJECT,
    ATTEND,
    SEND_ONE,
    NORM_TWO,
    TURN_TWO,
    ACTIVATE,
    MASK,
    GRAD_DOWN,
    BACK_HIDDEN,
    GRAD_UP,
    SEND_TWO,
    OUTPUT,
    SEND_THREE,
    BACK_TWO,
    TURN_BACK,
    GRAD_OUT,
    BACK_CONTEXT,
    ATTEND_BACK,
    GRAD_IN,
    SEND_FOUR,
    BACK_ONE,
) = range(23)
SCHEDULE = (
    (GATHER, 0, 0),
    (GATHER, 3, 0),
    (ROWS, TOKENS, 0),
    (GATHER, 7, 0),
    (GATHER, 0, 1),
    (GATHER, 0, 2),
    (GATHER, 3, 1),
    (GATHER, 3, 2),
    (GATHER, 2, 0),
    (GATHER, 7, 1),
    (GATHER, 6, 0),
    (GATHER, 1, 0),
    (GATHER, 8, 0),
    (GATHER, 7, 2),
    (ROWS, TOKENS, 1),
    (ROWS, TOKENS, 2),
    (COMPUTE, NORM_ONE, 0),
    (GATHER, 3, 3),
    (ROWS, COTANGENT, 0),
    (GATHER, 1, 1),
    (GATHER, 7, 3),
    (GATHER, 2, 1),
    (GATHER, 2, 2),
    (COMPUTE, TURN_ONE, 0),
    (GATHER, 0, 3),
    (GATHER, 8, 1),
    (GATHER, 9, 0),
    (GATHER, 1, 2),
    (GATHER, 1, 3),
    (GATHER, 2, 3),
    (GATHER, 8, 2),
    (GATHER, 8, 3),
    (GATHER, 4, 0),
    (GATHER, 4, 1),
    (GATHER, 3, 4),
    (GATHER, 0, 4),
    (GATHER, 7, 4),
    (GATHER, 9, 1),
    (GATHER, 9, 2),
    (GATHER, 10, 0),
    (COMPUTE, PROJECT, 2),
    (ROWS, COTANGENT, 1),
    (ROWS, COTANGENT, 2),
    (COMPUTE, MASK, 0),
    (GATHER, 2, 4),
    (COMPUTE, PROJECT, 1),
    (GATHER, 5, 0),
    (GATHER, 4, 2),
    (GATHER, 4, 3),
    (GATHER, 10, 1),
    (GATHER, 10, 2),
    (GATHER, 9, 3),
    (GATHER, 6, 1),
    (GATHER, 6, 2),
    (GATHER, 11, 0),
    (GATHER, 5, 1),
    (GATHER, 12, 0),
    (GATHER, 1, 4),
    (COMPUTE, PROJECT, 0),
    (COMPUTE, ATTEND, 0),
    (COMPUTE, ATTEND, 1),
    (COMPUTE, ATTEND, 2),
    (COMPUTE, ATTEND, 3),
    (GATHER, 5, 2),
    (GATHER, 5, 3),
    (GATHER, 11, 1),
    (GATHER, 6, 3),
    (GATHER, 12, 1),
    (GATHER, 4, 4),
    (COMPUTE, SEND_ONE, 0),
    (COMPUTE, NORM_TWO, 0),
    (COMPUTE, ACTIVATE, 2),
    (COMPUTE, GRAD_DOWN, 2),
    (SCATTER, 2, 0),
    (COMPUTE, TURN_TWO, 0),
    (GATHER, 5, 4),
    (COMPUTE, ACTIVATE, 0),
    (COMPUTE, GRAD_DOWN, 0),
    (SCATTER, 0, 0),
    (GATHER, 10, 3),
    (GATHER, 11, 2),
    (GATHER, 11, 3),
    (GATHER, 8, 4),
    (COMPUTE, ACTIVATE, 3),
    (COMPUTE, GRAD_DOWN, 3),
    (GATHER, 12, 2),
    (GATHER, 12, 3),
    (SCATTER, 2, 1),
    (GATHER, 9, 4),
    (COMPUTE, BACK_HIDDEN, 0),
    (COMPUTE, GRAD_UP, 0),
    (SCATTER, 4, 0),
    (GATHER, 6, 4),
    (COMPUTE, ACTIVATE, 1),
    (COMPUTE, GRAD_DOWN, 1),
    (SCATTER, 1, 0),
    (GATHER, 10, 4),
    (COMPUTE, BACK_HIDDEN, 1),
    (COMPUTE, GRAD_UP, 1),
    (SCATTER, 5, 0),
    (GATHER, 11, 4),
    (COMPUTE, BACK_HIDDEN, 2),
    (COMPUTE, GRAD_UP, 2),
    (SCATTER, 6, 0),
    (SCATTER, 0, 1),
    (GATHER, 12, 4),
    (COMPUTE, SEND_TWO, 0),
    (COMPUTE, BACK_HIDDEN, 3),
    (COMPUTE, GRAD_UP, 3),
    (SCATTER, 7, 0),
    (COMPUTE, OUTPUT, 0),
    (COMPUTE, SEND_THREE, 0),
    (ROWS, BLOCK, 0),
    (SCATTER, 3, 0),
    (SCATTER, 1, 1),
    (SCATTER, 2, 2),
    (SCATTER, 4, 1),
    (SCATTER, 0, 2),
    (COMPUTE, BACK_TWO, 0),
    (COMPUTE, BACK_CONTEXT, 0),
    (COMPUTE, ATTEND_BACK, 2),
    (COMPUTE, ATTEND_BACK, 1),
    (COMPUTE, TURN_BACK, 0),
    (SCATTER, 7, 1),
    (SCATTER, 6, 1),
    (COMPUTE, GRAD_OUT, 0),
    (SCATTER, 8, 0),
    (SCATTER, 1, 2),
    (SCATTER, 3, 1),
    (SCATTER, 5, 1),
    (SCATTER, 4, 2),
    (COMPUTE, ATTEND_BACK, 3),
    (COMPUTE, ATTEND_BACK, 0),
    (COMPUTE, GRAD_IN, 3),
    (SCATTER, 11, 0),
    (COMPUTE, SEND_FOUR, 0),
    (COMPUTE, GRAD_IN, 1),
    (COMPUTE, GRAD_IN, 5),
    (SCATTER, 13, 0),
    (SCATTER, 7, 2),
    (SCATTER, 8, 1),
    (SCATTER, 3, 2),
    (COMPUTE, GRAD_IN, 4),
    (SCATTER, 12, 0),
    (SCATTER, 6, 2),
    (SCATTER, 11, 1),
    (COMPUTE, GRAD_IN, 0),
    (SCATTER, 9, 0),
    (SCATTER, 5, 2),
    (COMPUTE, BACK_ONE, 0),
    (ROWS, GRADIENT, 0),
    (SMALL, 0, 0),
    (SMALL, 0, 1),
    (SCATTER, 8, 2),
    (SCATTER, 12, 1),
    (SCATTER, 9, 1),
    (COMPUTE, GRAD_IN, 2),
    (SCATTER, 10, 0),
    (SCATTER, 3, 3),
    (SCATTER, 13, 1),
    (SCATTER, 0, 3),
    (ROWS, BLOCK, 1),
    (SCATTER, 5, 3),
    (SCATTER, 11, 2),
    (SCATTER, 11, 3),
    (SMALL, 0, 2),
    (ROWS, GRADIENT, 1),
    (ROWS, GRADIENT, 2),
    (SCATTER, 7, 3),
    (SCATTER, 2, 3),
    (SCATTER, 12, 2),
    (SCATTER, 12, 3),
    (SCATTER, 9, 2),
    (SCATTER, 10, 1),
    (SCATTER, 6, 3),
    (SCATTER, 8, 3),
    (SCATTER, 8, 4),
    (SCATTER, 10, 2),
    (SCATTER, 1, 3),
    (SCATTER, 4, 3),
    (SCATTER, 13, 2),
    (SCATTER, 0, 4),
    (SCATTER, 10, 3),
    (SCATTER, 2, 4),
    (SMALL, 0, 3),
    (SCATTER, 3, 4),
    (SCATTER, 13, 3),
    (ROWS, BLOCK, 2),
    (SCATTER, 9, 3),
    (SCATTER, 1, 4),
    (SCATTER, 4, 4),
    (SCATTER, 7, 4),
    (SCATTER, 12, 4),
    (SCATTER, 5, 4),
    (SCATTER, 11, 4),
    (SCATTER, 10, 4),
    (SCATTER, 13, 4),
    (SCATTER, 6, 4),
    (SCATTER, 9, 4),
)


def nn(left, right):
    return jnp.dot(left, right, preferred_element_type=F32)


def nt(left, right):
    return lax.dot_general(left, right, (((1,), (1,)), ((), ())), preferred_element_type=F32)


def loop(count, body, start=0):
    def step(index, carry):
        body(index)
        return carry

    lax.fori_loop(start, count, step, 0)


def part(index, size):
    return pl.ds(pl.multiple_of(index * size, size), size)


def fold(block):
    return jnp.sum(block.reshape(-1, 8, block.shape[-1]), axis=0)


def layer_kernel(
    chain,
    tokens,
    cotangent,
    segments,
    weight_in,
    weight_out,
    weight_up,
    weight_down,
    first_gain,
    first_shift,
    input_bias,
    output_bias,
    second_gain,
    second_shift,
    up_bias,
    block_out,
    token_grad,
    in_sum,
    out_sum,
    up_sum,
    down_sum,
    small_out,
    store,
    over_b,
    over_rest,
    row_in,
    row_up,
    plain,
    first_t,
    second_t,
    up_t,
    heads,
    context,
    context_grad,
    residual,
    slope,
    hidden,
    send,
    recv,
    score,
    other,
    prob_low,
    flip,
    turned,
    gather_acc,
    log_sums,
    sums,
    up_sums,
    head_sums,
    small,
    small_x,
    small_y,
    small_z,
    keep_col,
    keep_row,
    peaks,
    block_sum,
    gather_send,
    gather_recv,
    local_sem,
    scatter_send,
    scatter_recv,
    pair_send,
    pair_recv,
    row_send,
    row_recv,
    small_send,
    small_recv,
):
    place = lax.axis_index("fsdp")
    y = lax.axis_index("context")
    t = lax.axis_index("tensor")
    z = place // 2
    x = place % 2
    half = chain // 2
    mine = x * 2 + y
    at_ab = (1 - x) * 2 + (1 - y)
    to_x = {"fsdp": z * 2 + (1 - x)}
    to_y = {"context": 1 - y}
    to_t = {"tensor": 1 - t}

    def sides(swapped):
        if swapped:
            return x * 2 + (1 - y), (1 - x) * 2 + y, to_y, to_x
        a_x = x + (1 - t) * (1 - 2 * x)
        a_y = y + t * (1 - 2 * y)
        b_x = x + t * (1 - 2 * x)
        b_y = y + (1 - t) * (1 - 2 * y)
        to_a = {"fsdp": z * 2 + a_x, "context": a_y}
        to_b = {"fsdp": z * 2 + b_x, "context": b_y}
        return a_x * 2 + a_y, b_x * 2 + b_y, to_a, to_b

    normal_sides = sides(0)
    swapped_sides = sides(1)

    near = 1 - z + 4 * (z // 2)
    mate = 3 - z
    far = 3 - near
    inner = ((z + 1) // 2) % 2 == 1
    outer = ((z + 1) // 2) % 2 == 0

    def to_z(k):
        return {"fsdp": k * 2 + x}

    def remote(source, target, send_sem, recv_sem, device):
        return pltpu.make_async_remote_copy(
            src_ref=source,
            dst_ref=target,
            send_sem=send_sem,
            recv_sem=recv_sem,
            device_id=device,
            device_id_type=MESH_ID,
        )

    slots = row_in.shape[0]
    own_slots = slots // 2
    quarter = own_slots // 2
    width = row_in.shape[1]

    shards = (
        [weight_in.at[k] for k in range(3)]
        + [weight_out]
        + [weight_up.at[:, k * COLS : (k + 1) * COLS] for k in range(4)]
        + [weight_down.at[:, k * COLS : (k + 1) * COLS] for k in range(4)]
    )
    rows = weight_out.shape[0]

    def load(j):
        return pltpu.make_async_copy(shards[j], store.at[j + 8 * (j // 8), z, mine], local_sem.at[j])

    for j in range(PIECES):
        load(j).start()

    barrier = pltpu.get_barrier_semaphore()
    for device in [to_x, to_y, to_t] + [to_z((z + step) % chain) for step in range(1, chain)]:
        pl.semaphore_signal(barrier, inc=1, device_id=device, device_id_type=MESH_ID)
    pl.semaphore_wait(barrier, chain + 2)

    def gathered(j, at, quarter_at):
        piece, start, count = GATHER_PIECES[j]
        return store.at[piece + 8 * (piece // 8), at, quarter_at, :, start : start + count]

    def gather_way(j):
        return swapped_sides if GATHER_SWAPPED[j] else normal_sides

    def gather_z(j, stream, source, slot, target):
        block = gathered(j, source, gather_way(j)[0] if stream else mine)
        return remote(
            block,
            block,
            gather_send.at[j, 4 * stream + slot],
            gather_recv.at[j, 4 * stream + source],
            to_z(target),
        )

    def gather_start(j, stream):
        gather_z(j, stream, z, 0, near).start()
        gather_z(j, stream, z, 1, mate).start()

        @pl.when(outer)
        def _():
            gather_z(j, stream, z, 2, far).start()

    def gather_pass(j, stream):
        @pl.when(inner)
        def _():
            gather_z(j, stream, mate, 0, z).wait_recv()
            gather_z(j, stream, mate, 3, near).start()

    def gather_end(j, stream):
        gather_z(j, stream, near, 0, z).wait_recv()
        gather_z(j, stream, far, 0, z).wait_recv()
        gather_z(j, stream, z, 0, near).wait_send()
        gather_z(j, stream, z, 1, mate).wait_send()

        @pl.when(outer)
        def _():
            gather_z(j, stream, mate, 0, z).wait_recv()
            gather_z(j, stream, z, 2, far).wait_send()

        @pl.when(inner)
        def _():
            gather_z(j, stream, z, 3, near).wait_send()

    def gather_side(j, kind):
        at_a, _, to_a, to_b = gather_way(j)
        everything = slice(None)
        if kind == 0:
            block, device = gathered(j, z if GATHER_KINDS[j] else everything, mine), to_a
        elif kind == 1:
            block, device = gathered(j, everything, mine), to_b
        else:
            block, device = gathered(j, everything, at_a), to_b
        return remote(block, block, gather_send.at[j, 8 + kind], gather_recv.at[j, 8 + kind], device)

    def gather_stage(j, stage):
        piece = GATHER_PIECES[j][0]
        if piece not in loaded:
            load(piece).wait()
            loaded.add(piece)
        if stage == 4:
            gather_side(j, 1).wait()
            gather_side(j, 2).wait()
        elif GATHER_KINDS[j]:
            if stage == 0:
                gather_side(j, 0).start()
                gather_start(j, 0)
            elif stage == 1:
                gather_side(j, 0).wait()
                gather_start(j, 1)
                gather_pass(j, 0)
            elif stage == 2:
                gather_pass(j, 1)
            else:
                gather_end(j, 0)
                gather_side(j, 1).start()
                gather_end(j, 1)
                gather_side(j, 2).start()
        elif stage == 0:
            gather_start(j, 0)
        elif stage == 1:
            gather_pass(j, 0)
        elif stage == 2:
            gather_end(j, 0)
            gather_side(j, 0).start()
            gather_side(j, 1).start()
        else:
            gather_side(j, 0).wait()
            gather_side(j, 2).start()

    def row_copies(source, target, which):
        mine_half = part(y, own_slots)
        local = pltpu.make_async_copy(source.at[y], target.at[mine_half], row_send.at[which, 2])
        place_there = pl.ds(pl.multiple_of(y * own_slots + t * quarter, quarter), quarter)
        across = remote(
            source.at[1 - y, part(t, quarter)],
            target.at[place_there],
            row_send.at[which, 0],
            row_recv.at[which, 0],
            to_y,
        )
        place_here = pl.ds(pl.multiple_of((1 - y) * own_slots + t * quarter, quarter), quarter)
        onward = remote(
            target.at[place_here], target.at[place_here], row_send.at[which, 1], row_recv.at[which, 1], to_t
        )
        return local, across, onward

    def row_back(source, target, which):
        mine_half = part(y, own_slots)
        local = pltpu.make_async_copy(source.at[mine_half], target.at[y], row_send.at[which, 2])
        from_here = pl.ds(pl.multiple_of((1 - y) * own_slots + t * quarter, quarter), quarter)
        across = remote(
            source.at[from_here],
            target.at[y, part(t, quarter)],
            row_send.at[which, 0],
            row_recv.at[which, 0],
            to_y,
        )
        block = target.at[1 - y, part(t, quarter)]
        onward = remote(block, block, row_send.at[which, 1], row_recv.at[which, 1], to_t)
        return local, across, onward

    token_local, token_across, token_on = row_copies(tokens, row_in, 0)
    up_local, up_across, up_on = row_copies(cotangent, row_up, 1)

    loaded = set()

    def stats(values):
        average = jnp.mean(values, axis=1, keepdims=True)
        centered = values - average
        inverse = lax.rsqrt(jnp.mean(centered * centered, axis=1, keepdims=True) + EPSILON)
        return centered * inverse, inverse

    norm_rows = 32

    def prepare():
        peaks[...] = jnp.full(peaks.shape, MASKED, F32)
        sums[...] = jnp.zeros(sums.shape, F32)
        keep_row[...] = jnp.where(segments[pl.ds(y, 1), :] > 0, 1.0, 0.0)
        keep_col[...] = jnp.broadcast_to(keep_row[...], (128, slots)).T

    def norm_first(i):
        at = part(i, norm_rows)
        scaled, _ = stats(row_in[at, :].astype(F32))
        plain[at, :] = (scaled * first_gain[...] + first_shift[...]).astype(BF)

    def turn(source, target):
        def body(j):
            target[part(j, 128), :] = source[:, part(j, 128)].T

        loop(width // 128, body)

    def project(c, which):
        at = part(c, TILE)
        tile = store[which, :, :, :, at].reshape(width, TILE)
        value = nn(plain[...], tile)
        if which != 1:
            value = value + input_bias[which // 2 : which // 2 + 1, at]
        heads[which, c] = value.astype(BF)

    lane = lax.broadcasted_iota(jnp.int32, (slots, 128), 1)
    chunk = 64
    n_chunks = slots // chunk

    def head_operands(pair, h):
        where_pair = part(pair % 2, 128)
        query = heads[0, pair // 2, :, where_pair].astype(F32) * (HEAD_DIM**-0.5)
        key = heads[1, pair // 2, :, where_pair].astype(F32)
        own = (lane < HEAD_DIM) if h == 0 else (lane >= HEAD_DIM)
        first = HEAD_DIM if h == 0 else 0
        flag = keep_col[:, 0:1]
        query = jnp.where(own, query, jnp.where(lane == first, flag, jnp.where(lane == first + 1, 1.0 - flag, 0.0)))
        key = jnp.where(
            lane == first, -BIG * (1.0 - flag), jnp.where(lane == first + 1, -BIG * flag, key)
        )
        return query.astype(BF), key.astype(BF), own

    def attend(pair):
        where_pair = part(pair % 2, 128)
        turned[...] = heads[2, pair // 2, :, where_pair].T
        for h in range(2):
            query, key, _ = head_operands(pair, h)
            score[...] = nt(key, query)

            def top(i, best):
                return jnp.maximum(best, jnp.max(score[part(i, chunk), :].reshape(-1, 8, slots), axis=0))

            best = lax.fori_loop(0, n_chunks, top, jnp.full((8, slots), -3e38, F32))
            highest = jnp.max(best, axis=0, keepdims=True)

            def power(i, total):
                at = part(i, chunk)
                powers = jnp.exp(score[at, :] - highest)
                prob_low[at, :] = powers.astype(BF)
                return total + fold(powers)

            total = lax.fori_loop(0, n_chunks, power, jnp.zeros((8, slots), F32))
            total = jnp.sum(total, axis=0, keepdims=True)
            mixed = nn(turned[h * HEAD_DIM : (h + 1) * HEAD_DIM, :], prob_low[...])
            flip[h * HEAD_DIM : (h + 1) * HEAD_DIM, :] = mixed / total
            log_sums[2 * pair + h] = highest + jnp.log(total)
            summit = jnp.max(jnp.where(keep_row[...] > 0.0, highest, MASKED), axis=1, keepdims=True)
            spots = lax.broadcasted_iota(jnp.int32, peaks.shape, 1)
            peaks[...] = jnp.where(spots == 2 * pair + h, summit, peaks[...])
        context[pair // 2, :, where_pair] = flip[...].T.astype(BF)

    def mask_rows(i):
        at = part(i, 64)
        row_up[at, :] = (row_up[at, :].astype(F32) * keep_col[at, 0:1]).astype(BF)

    def pair_copy(slot, j):
        return remote(send.at[j], recv.at[slot, j], pair_send.at[j], pair_recv.at[slot, j], to_t)

    def pair_sum(slot, product):
        def body(j):
            send[j] = product(j).astype(BF)
            pair_copy(slot, j).start()

        loop(4, body)

    def pair_wait(slot):
        for j in range(4):
            pair_copy(slot, j).wait()

    def summed(slot, at):
        return jnp.concatenate(
            [send[j, at, :].astype(F32) + recv[slot, j, at, :].astype(F32) for j in range(4)], axis=1
        )

    def weight_rows(piece, j, c):
        return store[piece, j, :, :, c * TILE : (c + 1) * TILE].reshape(TILE, TILE)

    def attended(j):
        return nt(context[0], weight_rows(3, j, 0)) + nt(context[1], weight_rows(3, j, 1))

    def norm_second(i):
        at = part(i, norm_rows)
        values = row_in[at, :].astype(F32) + summed(0, at) + output_bias[0:1, :]
        residual[at, :] = values
        scaled, _ = stats(values)
        plain[at, :] = (scaled * second_gain[...] + second_shift[...]).astype(BF)

    def activate(c):
        at = part(c % 2, TILE)
        tile = store[4 + c // 2, :, :, :, at].reshape(width, TILE)
        score[:, 0:TILE] = nn(plain[...], tile) + up_bias[0:1, part(c, TILE)]

        def rows_of(i):
            spot = part(i, 64)
            pre = score[spot, 0:TILE]
            chance = 0.5 * (1.0 + lax.erf(pre * HALF_ROOT))
            hidden[c, spot, :] = (pre * chance).astype(BF)
            slope[c, spot, :] = (chance + pre * jnp.exp(-0.5 * pre * pre) * DENSITY).astype(BF)

        loop(slots // 64, rows_of)

    def z_spot(p, stream, spot):
        return (stream if SCATTER_KINDS[p] else 1) * chain + spot

    def columns(p):
        _, start, count = SCATTER_PIECES[p]
        return slice(start, start + count)

    def scatter_way(p):
        return swapped_sides if SCATTER_SWAPPED[p] else normal_sides

    def partial(p, at, quarter_at):
        return store.at[8 + SCATTER_PIECES[p][0], at, quarter_at, :, columns(p)]

    def from_b(p, which, at):
        return over_b.at[SCATTER_PIECES[p][0], which, at, :, columns(p)]

    def from_rest(p, at):
        return over_rest.at[SCATTER_PIECES[p][0], at, :, columns(p)]

    def scatter_side(p, kind):
        at_a, at_b, to_a, to_b = scatter_way(p)
        sems = (scatter_send.at[p, kind], scatter_recv.at[p, kind])
        everything = slice(None)
        if kind == 0:
            return remote(partial(p, everything, at_b), from_b(p, 0, everything), *sems, to_b)
        if kind == 1:
            return remote(partial(p, everything, at_ab), from_b(p, 1, everything), *sems, to_b)
        if SCATTER_KINDS[p]:
            return remote(partial(p, z, at_a), from_rest(p, 2 * chain), *sems, to_a)
        return remote(partial(p, everything, at_a), from_rest(p, slice(0, chain)), *sems, to_a)

    def own_quarter(p, stream):
        return scatter_way(p)[0] if stream else mine

    def scatter_z(p, stream, slot, block, spot, target):
        return remote(
            partial(p, block, own_quarter(p, stream)),
            from_rest(p, z_spot(p, stream, spot)),
            scatter_send.at[p, 3 + 4 * stream + slot],
            scatter_recv.at[p, 3 + 4 * stream + spot],
            to_z(target),
        )

    def add_to(ref, *terms):
        total = ref[...].astype(F32)
        for term in terms:
            total = total + term[...].astype(F32)
        ref[...] = total.astype(BF)

    def scatter_start(p, stream):
        scatter_z(p, stream, 0, near, z, near).start()

        @pl.when(outer)
        def _():
            scatter_z(p, stream, 1, mate, z, mate).start()
            scatter_z(p, stream, 2, far, near, near).start()

        @pl.when(inner)
        def _():
            scatter_z(p, stream, 2, far, z, far).start()

    def scatter_pass(p, stream):
        @pl.when(inner)
        def _():
            scatter_z(p, stream, 0, near, z, near).wait_recv()
            add_to(partial(p, mate, own_quarter(p, stream)), from_rest(p, z_spot(p, stream, z)))
            scatter_z(p, stream, 1, mate, z, mate).start()

    def scatter_end(p, stream):
        scatter_z(p, stream, 0, near, near, near).wait_recv()
        scatter_z(p, stream, 0, near, mate, near).wait_recv()
        scatter_z(p, stream, 0, near, z, near).wait_send()
        scatter_z(p, stream, 1, mate, z, mate).wait_send()
        block_sum[:, columns(p)] = (
            partial(p, z, own_quarter(p, stream))[...].astype(F32)
            + from_rest(p, z_spot(p, stream, near))[...].astype(F32)
            + from_rest(p, z_spot(p, stream, mate))[...].astype(F32)
        )

        @pl.when(outer)
        def _():
            scatter_z(p, stream, 0, near, far, near).wait_recv()
            block_sum[:, columns(p)] += from_rest(p, z_spot(p, stream, far))[...].astype(F32)

        scatter_z(p, stream, 2, far, z, far).wait_send()

    def scatter_target(p):
        piece, start, count = SCATTER_PIECES[p]
        if piece < 4:
            return down_sum.at[:, piece * COLS + start : piece * COLS + start + count]
        if piece < 8:
            return up_sum.at[:, (piece - 4) * COLS + start : (piece - 4) * COLS + start + count]
        if piece == 8:
            return out_sum.at[:, start : start + count]
        return in_sum.at[piece - 9, :, start : start + count]

    def scatter_stage(p, stage):
        late = SCATTER_KINDS[p]
        at_a = scatter_way(p)[0]
        if stage == 0:
            scatter_side(p, 0).start()
            scatter_side(p, 1).start()
        elif stage == 1:
            scatter_side(p, 0).wait()
            scatter_side(p, 1).wait()

            def body(k):
                add_to(partial(p, k, mine), from_b(p, 0, k))
                add_to(partial(p, k, at_a), from_b(p, 1, k))

            loop(chain, body)
            if late:
                scatter_start(p, 0)
                scatter_start(p, 1)
            else:
                scatter_side(p, 2).start()
        elif stage == 2:
            if late:
                scatter_pass(p, 0)
                scatter_pass(p, 1)
            else:
                scatter_side(p, 2).wait()
                loop(chain, lambda k: add_to(partial(p, k, mine), from_rest(p, k)))
                scatter_start(p, 0)
        elif stage == 3:
            if late:
                scatter_end(p, 1)
                partial(p, z, at_a)[...] = block_sum[:, columns(p)].astype(BF)
                scatter_side(p, 2).start()
            else:
                scatter_pass(p, 0)
        else:
            scatter_end(p, 0)
            total = block_sum[:, columns(p)]
            if late:
                scatter_side(p, 2).wait()
                total = total + from_rest(p, 2 * chain)[...].astype(F32)
            scatter_target(p)[...] = total

    def gradient(left, right, piece, c):
        def body(m):
            block = nn(left[part(m, width // 2), :], right)
            store[8 + piece, part(m, half), :, :, part(c, TILE)] = block.astype(BF).reshape(half, 4, rows, TILE)

        loop(2, body)

    def back_hidden(c):
        at = part(c % 2, TILE)
        tile = store[16 + c // 2, :, :, :, at].reshape(width, TILE)
        score[:, 0:TILE] = nn(row_up[...], tile)

        def rows_of(i, total):
            spot = part(i, 64)
            grad = (score[spot, 0:TILE] * slope[c, spot, :].astype(F32)).astype(BF)
            slope[c, spot, :] = grad
            return total + fold(grad.astype(F32))

        total = lax.fori_loop(0, slots // 64, rows_of, jnp.zeros((8, TILE), F32))
        up_sums[c] = jnp.sum(total, axis=0, keepdims=True)

    def mixed(j):
        total = nt(hidden[0], weight_rows(16, j, 0))
        for c in range(1, 8):
            total = total + nt(hidden[c], weight_rows(16 + c // 2, j, c % 2))
        return total

    def output_rows(i):
        at = part(i, norm_rows)
        values = residual[at, :] + summed(1, at) + output_bias[1:2, :]
        plain[at, :] = (values * keep_col[at, 0:1]).astype(BF)

    block_local, block_across, block_on = row_back(plain, block_out, 2)

    def second_back(j):
        total = nt(slope[0], weight_rows(4, j, 0))
        for c in range(1, 8):
            total = total + nt(slope[c], weight_rows(4 + c // 2, j, c % 2))
        return total

    def norm_second_back(i):
        at = part(i, norm_rows)
        scaled, inverse = stats(residual[at, :])
        incoming = summed(0, at)
        weighted = incoming * second_gain[...]
        upstream = row_up[at, :].astype(F32)
        bracket = (
            weighted
            - jnp.mean(weighted, axis=1, keepdims=True)
            - scaled * jnp.mean(weighted * scaled, axis=1, keepdims=True)
        )
        total = upstream + inverse * bracket
        residual[at, :] = total
        low = total.astype(BF)
        for j in range(4):
            hidden[4 + j, at, :] = low[:, j * TILE : (j + 1) * TILE]
        sums[0] += fold(incoming * scaled)
        sums[1] += fold(incoming)
        sums[2] += fold(total)
        sums[3] += fold(upstream)

    def turn_attend():
        for j in range(4):
            for k in range(2):
                at = j * TILE + k * 128
                up_t[at : at + 128, :] = hidden[4 + j, :, k * 128 : (k + 1) * 128].T

    def back_context(c):
        total = None
        for j in range(4):
            tile = store[3, j, :, :, part(c, TILE)].reshape(TILE, TILE)
            term = nn(hidden[4 + j], tile)
            total = term if total is None else total + term
        context_grad[c] = total.astype(BF)

    def attend_back(pair):
        where_pair = part(pair % 2, 128)
        turned[...] = heads[1, pair // 2, :, where_pair].T
        value = heads[2, pair // 2, :, where_pair]
        incoming = context_grad[pair // 2, :, where_pair]
        for h in range(2):
            query, key, own = head_operands(pair, h)
            own_in = jnp.where(own, incoming.astype(F32), 0.0).astype(BF)
            score[...] = nt(key, query)
            other[...] = nt(value, own_in)
            logs = log_sums[2 * pair + h]

            def power(i, total):
                at = part(i, chunk)
                probs = jnp.exp(score[at, :] - logs)
                score[at, :] = probs
                prob_low[at, :] = probs.astype(BF)
                return total + fold(probs * other[at, :])

            total = lax.fori_loop(0, n_chunks, power, jnp.zeros((8, slots), F32))
            centre = jnp.sum(total, axis=0, keepdims=True)

            value_grad = nn(prob_low[...], own_in)

            def rest(i):
                at = part(i, chunk)
                prob_low[at, :] = (score[at, :] * (other[at, :] - centre)).astype(BF)

            loop(n_chunks, rest)
            key_grad = nn(prob_low[...], query)
            if h == 0:
                gather_acc[0] = value_grad
                gather_acc[1] = key_grad
            else:
                gather_acc[0] += value_grad
                gather_acc[1] = jnp.where(own, key_grad, gather_acc[1])
            flip[h * HEAD_DIM : (h + 1) * HEAD_DIM, :] = nn(
                turned[h * HEAD_DIM : (h + 1) * HEAD_DIM, :], prob_low[...]
            ) * (HEAD_DIM**-0.5)
        query_low = flip[...].T.astype(BF)
        value_low = gather_acc[0].astype(BF)
        heads[0, pair // 2, :, where_pair] = query_low
        heads[1, pair // 2, :, where_pair] = gather_acc[1].astype(BF)
        heads[2, pair // 2, :, where_pair] = value_low
        head_sums[0, pair] = jnp.sum(query_low.astype(F32), axis=0, keepdims=True)
        head_sums[1, pair] = jnp.sum(value_low.astype(F32), axis=0, keepdims=True)

    def first_back(j):
        total = None
        for i in range(3):
            for c in range(2):
                term = nt(heads[i, c], weight_rows(i, j, c))
                total = term if total is None else total + term
        return total

    def norm_first_back(i):
        at = part(i, norm_rows)
        scaled, inverse = stats(row_in[at, :].astype(F32))
        incoming = summed(1, at)
        weighted = incoming * first_gain[...]
        bracket = (
            weighted
            - jnp.mean(weighted, axis=1, keepdims=True)
            - scaled * jnp.mean(weighted * scaled, axis=1, keepdims=True)
        )
        row_in[at, :] = (residual[at, :] + inverse * bracket).astype(BF)
        sums[4] += fold(incoming * scaled)
        sums[5] += fold(incoming)

    grad_local, grad_across, grad_on = row_back(row_in, token_grad, 3)

    def collapse(k):
        return jnp.sum(sums[k], axis=0, keepdims=True)

    def small_fill():
        small[0:1, :] = collapse(4)
        small[1:2, :] = collapse(5)
        small[2:3, :] = jnp.concatenate([head_sums[i, k] for i in range(2) for k in range(4)], axis=1)
        small[3:4, :] = collapse(2)
        small[4:5, :] = collapse(3)
        small[5:6, :] = collapse(0)
        small[6:7, :] = collapse(1)
        small[7:8, :] = jnp.concatenate([up_sums[k] for k in range(4)], axis=1)
        small[8:9, :] = jnp.concatenate([up_sums[4 + k] for k in range(4)], axis=1)
        small[9:10, :] = jnp.concatenate([peaks[0:1, :]] * 8, axis=1)
        small[10:16, :] = jnp.zeros((6, small.shape[1]), F32)

    row_index = lax.broadcasted_iota(jnp.int32, small.shape, 0)

    def joined(left, right):
        return jnp.where(row_index == 9, jnp.maximum(left, right), left + right)

    def small_copy(source, target, k, device):
        return remote(source, target, small_send.at[k], small_recv.at[k], device)

    over_x = small_copy(small, small_x.at[0], 0, to_x)
    over_y = small_copy(small_x.at[1], small_y, 1, to_y)
    along_z = [
        small_copy(small_z.at[z], small_z.at[z], 1 + step, to_z((z + step) % chain)) for step in range(1, chain)
    ]

    def small_stage(stage):
        if stage == 0:
            small_fill()
            over_x.start()
        elif stage == 1:
            over_x.wait()
            small_x[1] = joined(small[...], small_x[0])
            over_y.start()
        elif stage == 2:
            over_y.wait()
            small_z[z] = joined(small_x[1], small_y[...])
            for copy in along_z:
                copy.start()
        else:
            for copy in along_z:
                copy.wait()
            total = small_z[0]
            for k in range(1, chain):
                total = joined(total, small_z[k])
            small_out[...] = total

    rows_over = {
        TOKENS: (token_local, token_across, token_on),
        COTANGENT: (up_local, up_across, up_on),
        BLOCK: (block_local, block_across, block_on),
        GRADIENT: (grad_local, grad_across, grad_on),
    }

    def rows_stage(which, stage):
        local, across, onward = rows_over[which]
        if stage == 0:
            local.start()
            across.start()
        elif stage == 1:
            across.wait()
            onward.start()
        else:
            onward.wait()
            local.wait()

    def norms(slot, body):
        pair_wait(slot)
        loop(slots // norm_rows, body)

    def mask_and_turn():
        loop(slots // 64, mask_rows)
        turn(row_up, up_t)

    compute = {
        NORM_ONE: lambda i: (prepare(), loop(slots // norm_rows, norm_first)),
        TURN_ONE: lambda i: turn(plain, first_t),
        PROJECT: lambda i: loop(2, lambda c: project(c, i)),
        ATTEND: attend,
        SEND_ONE: lambda i: pair_sum(0, attended),
        NORM_TWO: lambda i: norms(0, norm_second),
        TURN_TWO: lambda i: turn(plain, second_t),
        ACTIVATE: lambda i: loop(2 * i + 2, activate, 2 * i),
        MASK: lambda i: mask_and_turn(),
        GRAD_DOWN: lambda i: loop(2, lambda c: gradient(up_t, hidden[2 * i + c], i, c)),
        BACK_HIDDEN: lambda i: loop(2 * i + 2, back_hidden, 2 * i),
        GRAD_UP: lambda i: loop(2, lambda c: gradient(second_t, slope[2 * i + c], 4 + i, c)),
        SEND_TWO: lambda i: pair_sum(1, mixed),
        OUTPUT: lambda i: norms(1, output_rows),
        SEND_THREE: lambda i: pair_sum(0, second_back),
        BACK_TWO: lambda i: norms(0, norm_second_back),
        TURN_BACK: lambda i: turn_attend(),
        GRAD_OUT: lambda i: loop(2, lambda c: gradient(up_t, context[c], 8, c)),
        BACK_CONTEXT: lambda i: loop(2, back_context),
        ATTEND_BACK: attend_back,
        GRAD_IN: lambda i: gradient(first_t, heads[i // 2, i % 2], 9 + i // 2, i % 2),
        SEND_FOUR: lambda i: pair_sum(1, first_back),
        BACK_ONE: lambda i: norms(1, norm_first_back),
    }
    for kind, which, index in SCHEDULE:
        if kind == GATHER:
            gather_stage(which, index)
        elif kind == SCATTER:
            scatter_stage(which, index)
        elif kind == ROWS:
            rows_stage(which, index)
        elif kind == SMALL:
            small_stage(index)
        else:
            compute[which](index)


def finish_kernel(
    block_in,
    grad_in,
    in_sum,
    out_sum,
    up_sum,
    down_sum,
    small,
    weight,
    block_out,
    grad_out,
    first_gain,
    first_shift,
    in_out,
    in_bias,
    out_out,
    out_bias,
    second_gain,
    second_shift,
    up_out,
    up_bias,
    down_out,
    clipped,
    factor,
):
    block_out[...] = block_in[...]
    grad_out[...] = grad_in[...].astype(F32)
    out_out[...] = out_sum[...]
    up_out[...] = up_sum[...]
    down_out[...] = down_sum[...]
    local = out_sum.shape[1]
    in_out[...] = in_sum[...]
    first_gain[...] = small[0, :]
    first_shift[...] = small[1, :]
    in_bias[0:1, :] = small[2:3, 0:local]
    in_bias[1:2, :] = small[2:3, local:]
    out_bias[...] = small[3:5, :]
    second_gain[...] = small[5, :]
    second_shift[...] = small[6, :]
    width = small.shape[1]
    up_bias[0:width] = small[7, :]
    up_bias[width:] = small[8, :]
    factors = CLIP_LIMIT / jnp.maximum(small[9:10, 0:128], CLIP_LIMIT)
    factor[...] = factors[0, 0 : factor.shape[0]]
    roots = jnp.sqrt(factors)
    head = lax.broadcasted_iota(jnp.int32, (1, local), 1) // HEAD_DIM
    scale = jnp.zeros((1, local), F32)
    for h in range(local // HEAD_DIM):
        scale = jnp.where(head == h, roots[:, h : h + 1], scale)
    for k in range(2):
        clipped[:, k, :] = weight[k].astype(F32) * scale


def on_device_fused(
    tokens,
    segments,
    first_gain,
    first_shift,
    input_weight,
    input_bias,
    output_weight,
    output_bias,
    second_gain,
    second_shift,
    up_weight,
    up_bias,
    down_weight,
    cotangent,
    chain,
):
    group, tok_rows, width = tokens.shape
    slots = segments.shape[1]
    rows = input_weight.shape[0]
    weights = jnp.transpose(input_weight, (1, 0, 2))
    operands = (
        tokens,
        cotangent,
        segments,
        weights,
        output_weight,
        up_weight,
        down_weight,
        first_gain[None],
        first_shift[None],
        input_bias,
        output_bias,
        second_gain[None],
        second_shift[None],
        up_bias[None],
    )
    anywhere = pl.BlockSpec(memory_space=pl.ANY)
    vmem = pl.BlockSpec(memory_space=pltpu.VMEM)
    block = (rows, COLS)
    dma = pltpu.SemaphoreType.DMA
    results = pl.pallas_call(
        functools.partial(layer_kernel, chain),
        out_shape=(
            jax.ShapeDtypeStruct(tokens.shape, BF),
            jax.ShapeDtypeStruct(tokens.shape, BF),
            jax.ShapeDtypeStruct((3, rows, COLS), F32),
            jax.ShapeDtypeStruct((rows, COLS), F32),
            jax.ShapeDtypeStruct((rows, 4 * COLS), F32),
            jax.ShapeDtypeStruct((rows, 4 * COLS), F32),
            jax.ShapeDtypeStruct((16, width), F32),
        ),
        in_specs=[anywhere] * 2 + [vmem] + [anywhere] * 4 + [vmem] * 7,
        out_specs=[anywhere] * 2 + [vmem] * 5,
        scratch_shapes=[
            pltpu.VMEM((20, chain, 4) + block, BF),
            pltpu.VMEM((PIECES, 2, chain) + block, BF),
            pltpu.VMEM((PIECES, 2 * chain + 1) + block, BF),
            pltpu.VMEM((slots, width), BF),
            pltpu.VMEM((slots, width), BF),
            pltpu.VMEM((slots, width), BF),
            pltpu.VMEM((width, slots), BF),
            pltpu.VMEM((width, slots), BF),
            pltpu.VMEM((width, slots), BF),
            pltpu.VMEM((3, 2, slots, TILE), BF),
            pltpu.VMEM((2, slots, TILE), BF),
            pltpu.VMEM((2, slots, TILE), BF),
            pltpu.VMEM((slots, width), F32),
            pltpu.VMEM((8, slots, TILE), BF),
            pltpu.VMEM((8, slots, TILE), BF),
            pltpu.VMEM((4, slots, TILE), BF),
            pltpu.VMEM((2, 4, slots, TILE), BF),
            pltpu.VMEM((slots, slots), F32),
            pltpu.VMEM((slots, slots), F32),
            pltpu.VMEM((slots, slots), BF),
            pltpu.VMEM((128, slots), F32),
            pltpu.VMEM((128, slots), BF),
            pltpu.VMEM((2, slots, 128), F32),
            pltpu.VMEM((8, 1, slots), F32),
            pltpu.VMEM((6, 8, width), F32),
            pltpu.VMEM((8, 1, TILE), F32),
            pltpu.VMEM((2, 4, 1, 128), F32),
            pltpu.VMEM((16, width), F32),
            pltpu.VMEM((2, 16, width), F32),
            pltpu.VMEM((16, width), F32),
            pltpu.VMEM((chain, 16, width), F32),
            pltpu.VMEM((slots, 128), F32),
            pltpu.VMEM((1, slots), F32),
            pltpu.VMEM((8, 128), F32),
            pltpu.VMEM(block, F32),
            dma((len(GATHER_PIECES), 11)),
            dma((len(GATHER_PIECES), 11)),
            dma((PIECES,)),
            dma((len(SCATTER_PIECES), 11)),
            dma((len(SCATTER_PIECES), 11)),
            dma((4,)),
            dma((2, 4)),
            dma((4, 3)),
            dma((4, 2)),
            dma((2 + chain,)),
            dma((2 + chain,)),
        ],
        compiler_params=pltpu.CompilerParams(
            collective_id=0, has_side_effects=True, vmem_limit_bytes=67043328
        ),
        name="layer",
    )(*operands)
    local = input_weight.shape[2]
    flat = jax.ShapeDtypeStruct((width,), F32)
    finished = pl.pallas_call(
        finish_kernel,
        out_shape=(
            jax.ShapeDtypeStruct(tokens.shape, BF),
            jax.ShapeDtypeStruct(tokens.shape, F32),
            flat,
            flat,
            jax.ShapeDtypeStruct(weights.shape, F32),
            jax.ShapeDtypeStruct(input_bias.shape, F32),
            jax.ShapeDtypeStruct((rows, local), F32),
            jax.ShapeDtypeStruct(output_bias.shape, F32),
            flat,
            flat,
            jax.ShapeDtypeStruct(up_weight.shape, F32),
            jax.ShapeDtypeStruct(up_bias.shape, F32),
            jax.ShapeDtypeStruct(down_weight.shape, F32),
            jax.ShapeDtypeStruct((rows, 2, local), F32),
            jax.ShapeDtypeStruct((local // HEAD_DIM,), F32),
        ),
        in_specs=[vmem] * 8,
        out_specs=[vmem] * 15,
        name="finish",
    )(*results, weights)
    return finished[:4] + (jnp.transpose(finished[4], (1, 0, 2)),) + finished[5:]


def on_device(
    tokens,
    segments,
    first_gain,
    first_shift,
    input_weight,
    input_bias,
    output_weight,
    output_bias,
    second_gain,
    second_shift,
    up_weight,
    up_bias,
    down_weight,
    cotangent,
):
    group = tokens.shape[0]
    tok_rows = tokens.shape[1]
    width = tokens.shape[2]
    score_scale = HEAD_DIM ** (-0.5)
    position = lax.axis_index("context") * tok_rows
    query_segments = lax.dynamic_slice_in_dim(segments, position, tok_rows, 1)
    allowed = segments[:, None, :] == query_segments[:, :, None]
    real_pairs = allowed & (query_segments[:, :, None] > 0)
    keep_rows = (query_segments > 0).astype(jnp.float32).reshape(-1)[:, None]
    input_full, output_full = (
        lax.all_gather(input_weight, ("fsdp", "context"), axis=0, tiled=True),
        lax.all_gather(output_weight, ("fsdp", "context"), axis=0, tiled=True),
    )
    tokens_float = tokens.astype(jnp.float32).reshape(group * tok_rows, width)
    normed_one, scaled_one, inverse_one = normalize(tokens_float, first_gain, first_shift)
    first_operand = normed_one.astype(jnp.bfloat16)
    projected = jnp.einsum(
        "td,dcf->tcf", first_operand, input_full, preferred_element_type=jnp.float32
    )
    bias_rows = jnp.stack([input_bias[0], jnp.zeros_like(input_bias[0]), input_bias[1]])
    projected = (projected + bias_rows[None]).astype(jnp.bfloat16)
    local_width = projected.shape[2]
    projected = projected.reshape(group, tok_rows, 3, local_width)
    sources = lax.all_gather(projected[:, :, 1:], "context", axis=1, tiled=True)
    query_heads = split_heads(projected[:, :, 0])
    key_heads = split_heads(sources[:, :, 0])
    value_heads = split_heads(sources[:, :, 1])

    def head_forward(operands):
        query_one, key_one, value_one = operands
        logits = (
            jnp.einsum("gqd,gkd->gqk", query_one, key_one, preferred_element_type=jnp.float32)
            * score_scale
        )
        masked = jnp.where(allowed, logits, MASKED)
        summit = jnp.max(jnp.where(real_pairs, logits, MASKED))
        highest = jnp.max(masked, axis=2, keepdims=True)
        powers = jnp.exp(masked - highest)
        totals = jnp.sum(powers, axis=2, keepdims=True)
        weights_low = (powers / totals).astype(jnp.bfloat16)
        mixed = jnp.einsum(
            "gqk,gkd->gqd", weights_low, value_one, preferred_element_type=jnp.float32
        )
        return (mixed.astype(jnp.bfloat16), (highest + jnp.log(totals))[:, :, 0], summit)

    head_context, log_totals, summits = lax.map(head_forward, (query_heads, key_heads, value_heads))
    context = join_heads(head_context).reshape(group * tok_rows, local_width)
    attended = lax.psum(
        jnp.einsum("tf,df->td", context, output_full, preferred_element_type=jnp.float32), "tensor"
    )
    residual = tokens_float + attended + output_bias[0]
    peaks = lax.pmax(summits, ("fsdp", "context"))
    up_full, down_full = (
        lax.all_gather(up_weight, ("fsdp", "context"), axis=0, tiled=True),
        lax.all_gather(down_weight, ("fsdp", "context"), axis=0, tiled=True),
    )
    normed_two, scaled_two, inverse_two = normalize(residual, second_gain, second_shift)
    second_operand = normed_two.astype(jnp.bfloat16)
    pre_act = jnp.dot(second_operand, up_full, preferred_element_type=jnp.float32) + up_bias
    hidden = jax.nn.gelu(pre_act, approximate=False).astype(jnp.bfloat16)
    mixed_sum = lax.psum(
        jnp.einsum("tf,df->td", hidden, down_full, preferred_element_type=jnp.float32).astype(
            jnp.bfloat16
        ),
        "tensor",
    ).astype(jnp.float32)
    block_output = ((residual + mixed_sum + output_bias[1]) * keep_rows).astype(jnp.bfloat16)
    factor = CLIP_LIMIT / jnp.maximum(peaks, CLIP_LIMIT)
    column_scale = jnp.repeat(jnp.sqrt(factor), HEAD_DIM)
    clipped_weight = input_weight[:, :2, :].astype(jnp.float32) * column_scale[None, None, :]
    input_full, output_full, up_full, down_full = (
        lax.all_gather(input_weight, ("fsdp", "context"), axis=0, tiled=True),
        lax.all_gather(output_weight, ("fsdp", "context"), axis=0, tiled=True),
        lax.all_gather(up_weight, ("fsdp", "context"), axis=0, tiled=True),
        lax.all_gather(down_weight, ("fsdp", "context"), axis=0, tiled=True),
    )
    upstream = cotangent.astype(jnp.float32).reshape(group * tok_rows, width) * keep_rows
    upstream_low = upstream.astype(jnp.bfloat16)
    down_gradient = jnp.einsum(
        "td,tf->df", upstream_low, hidden, preferred_element_type=jnp.float32
    )
    pre_gradient = (
        jnp.dot(upstream_low, down_full, preferred_element_type=jnp.float32) * gelu_slope(pre_act)
    ).astype(jnp.bfloat16)
    up_gradient = jnp.einsum(
        "td,tf->df", second_operand, pre_gradient, preferred_element_type=jnp.float32
    )
    up_bias_gradient = jnp.sum(pre_gradient.astype(jnp.float32), axis=0)
    second_gradient = lax.psum(
        jnp.einsum("tf,df->td", pre_gradient, up_full, preferred_element_type=jnp.float32), "tensor"
    )
    through_two, second_gain_gradient, second_shift_gradient = normalize_back(
        second_gradient, scaled_two, inverse_two, second_gain
    )
    residual_gradient = upstream + through_two
    output_bias_gradient = jnp.stack(
        [jnp.sum(residual_gradient, axis=0), jnp.sum(upstream, axis=0)]
    )
    attend_low = residual_gradient.astype(jnp.bfloat16)
    output_gradient = jnp.einsum(
        "td,tf->df", attend_low, context, preferred_element_type=jnp.float32
    )
    context_back = jnp.dot(attend_low, output_full, preferred_element_type=jnp.float32).astype(
        jnp.bfloat16
    )
    context_gradient = split_heads(context_back.reshape(group, tok_rows, local_width))

    def head_backward(operands):
        query_one, key_one, value_one, incoming, log_total = operands
        logits = (
            jnp.einsum("gqd,gkd->gqk", query_one, key_one, preferred_element_type=jnp.float32)
            * score_scale
        )
        probs = jnp.exp(jnp.where(allowed, logits, MASKED) - log_total[:, :, None])
        prob_gradient = jnp.einsum(
            "gqd,gkd->gqk", incoming, value_one, preferred_element_type=jnp.float32
        )
        centre = jnp.sum(probs * prob_gradient, axis=2, keepdims=True)
        score_low = (probs * (prob_gradient - centre) * score_scale).astype(jnp.bfloat16)
        query_gradient = jnp.einsum(
            "gqk,gkd->gqd", score_low, key_one, preferred_element_type=jnp.float32
        ).astype(jnp.bfloat16)
        key_gradient = jnp.einsum(
            "gqk,gqd->gkd", score_low, query_one, preferred_element_type=jnp.float32
        )
        value_gradient = jnp.einsum(
            "gqk,gqd->gkd", probs.astype(jnp.bfloat16), incoming, preferred_element_type=jnp.float32
        )
        return (query_gradient, key_gradient, value_gradient)

    query_grads, key_grads, value_grads = lax.map(
        head_backward, (query_heads, key_heads, value_heads, context_gradient, log_totals)
    )
    source_terms = jnp.stack([join_heads(key_grads), join_heads(value_grads)], axis=2)
    source_sums = lax.psum_scatter(
        source_terms.astype(jnp.bfloat16), "context", scatter_dimension=1, tiled=True
    )
    source_low = source_sums.reshape(group * tok_rows, 2, local_width)
    query_flat = join_heads(query_grads).reshape(group * tok_rows, local_width)
    projected_gradient = jnp.concatenate([query_flat[:, None, :], source_low], axis=1)
    input_gradient = jnp.einsum(
        "td,tcf->dcf", first_operand, projected_gradient, preferred_element_type=jnp.float32
    )
    input_bias_gradient = jnp.stack(
        [
            jnp.sum(projected_gradient[:, 0].astype(jnp.float32), axis=0),
            jnp.sum(projected_gradient[:, 2].astype(jnp.float32), axis=0),
        ]
    )
    first_gradient = lax.psum(
        jnp.einsum(
            "tcf,dcf->td", projected_gradient, input_full, preferred_element_type=jnp.float32
        ).astype(jnp.bfloat16),
        "tensor",
    ).astype(jnp.float32)
    through_one, first_gain_gradient, first_shift_gradient = normalize_back(
        first_gradient, scaled_one, inverse_one, first_gain
    )
    tokens_gradient = (residual_gradient + through_one).reshape(group, tok_rows, width)
    block_output = block_output.reshape(group, tok_rows, width)
    (
        first_gain_sum,
        first_shift_sum,
        input_bias_sum,
        output_bias_sum,
        second_gain_sum,
        second_shift_sum,
        up_bias_sum,
    ) = lax.psum(
        (
            first_gain_gradient,
            first_shift_gradient,
            input_bias_gradient,
            output_bias_gradient,
            second_gain_gradient,
            second_shift_gradient,
            up_bias_gradient,
        ),
        ("fsdp", "context"),
    )
    input_sum, output_sum, up_sum, down_sum = (
        lax.psum_scatter(input_gradient, ("fsdp", "context"), scatter_dimension=0, tiled=True),
        lax.psum_scatter(output_gradient, ("fsdp", "context"), scatter_dimension=0, tiled=True),
        lax.psum_scatter(up_gradient, ("fsdp", "context"), scatter_dimension=0, tiled=True),
        lax.psum_scatter(down_gradient, ("fsdp", "context"), scatter_dimension=0, tiled=True),
    )
    return (
        block_output,
        tokens_gradient,
        first_gain_sum,
        first_shift_sum,
        input_sum,
        input_bias_sum,
        output_sum,
        output_bias_sum,
        second_gain_sum,
        second_shift_sum,
        up_sum,
        up_bias_sum,
        down_sum,
        clipped_weight,
        factor,
    )


def solution(mesh):
    placed = (
        P("fsdp", "context", None),
        P("fsdp", None),
        P(),
        P(),
        P(("fsdp", "context"), None, "tensor"),
        P(None, "tensor"),
        P(("fsdp", "context"), "tensor"),
        P(),
        P(),
        P(),
        P(("fsdp", "context"), "tensor"),
        P("tensor"),
        P(("fsdp", "context"), "tensor"),
        P("fsdp", "context", None),
    )
    chain = mesh.shape["fsdp"] // 2
    step = on_device
    if mesh.shape["context"] == 2 and mesh.shape["tensor"] == 2 and chain == 4:
        step = functools.partial(on_device_fused, chain=chain)
    return jax.shard_map(
        step,
        mesh=mesh,
        in_specs=placed,
        out_specs=(
            P("fsdp", "context", None),
            P("fsdp", "context", None),
            P(),
            P(),
            P(("fsdp", "context"), None, "tensor"),
            P(None, "tensor"),
            P(("fsdp", "context"), "tensor"),
            P(),
            P(),
            P(),
            P(("fsdp", "context"), "tensor"),
            P("tensor"),
            P(("fsdp", "context"), "tensor"),
            P(("fsdp", "context"), None, "tensor"),
            P("tensor"),
        ),
        check_vma=False,
    )
```

```python
import functools

import jax
import jax.numpy as jnp
from jax import lax
from jax.experimental import pallas as pl
from jax.experimental.pallas import tpu as pltpu
from jax.sharding import PartitionSpec as P

HEAD_DIM = 64


EPSILON = 1e-06
CLIP_LIMIT = 1.5
MASKED = -1e30
HALF_ROOT = 0.7071067811865476
DENSITY = 0.3989422804014327


def normalize(values, gain, shift):
    average = jnp.mean(values, axis=-1, keepdims=True)
    centered = values - average
    inverse = lax.rsqrt(jnp.mean(centered * centered, axis=-1, keepdims=True) + EPSILON)
    scaled = centered * inverse
    return (scaled * gain + shift, scaled, inverse)


def normalize_back(incoming, scaled, inverse, gain):
    weighted = incoming * gain
    bracket = (
        weighted
        - jnp.mean(weighted, axis=-1, keepdims=True)
        - scaled * jnp.mean(weighted * scaled, axis=-1, keepdims=True)
    )
    return (inverse * bracket, jnp.sum(incoming * scaled, axis=0), jnp.sum(incoming, axis=0))


def gelu_slope(values):
    return (
        0.5 * (1.0 + lax.erf(values * HALF_ROOT))
        + values * jnp.exp(-0.5 * values * values) * DENSITY
    )


def split_heads(values):
    shaped = values.reshape(values.shape[0], values.shape[1], -1, HEAD_DIM)
    return jnp.transpose(shaped, (2, 0, 1, 3))


def join_heads(values):
    moved = jnp.transpose(values, (1, 2, 0, 3))
    return moved.reshape(moved.shape[0], moved.shape[1], -1)


BF = jnp.bfloat16
F32 = jnp.float32
COLS = 512
TILE = 256
PIECES = 12
BIG = 1e30
MESH_ID = pl.DeviceIdType.MESH
GATHER_PIECES = (
    (0, 0, 256),
    (0, 256, 256),
    (1, 0, 512),
    (2, 0, 512),
    (3, 0, 512),
    (4, 0, 512),
    (5, 0, 512),
    (6, 0, 512),
    (7, 0, 512),
    (8, 0, 512),
    (9, 0, 512),
    (10, 0, 512),
    (11, 0, 512),
)
SCATTER_PIECES = (
    (0, 0, 512),
    (1, 0, 512),
    (2, 0, 512),
    (3, 0, 512),
    (4, 0, 512),
    (5, 0, 512),
    (6, 0, 512),
    (7, 0, 512),
    (8, 0, 512),
    (9, 0, 512),
    (10, 0, 256),
    (10, 256, 256),
    (11, 0, 256),
    (11, 256, 256),
)
GATHER_KINDS = (0, 0, 0, 0, 0, 1, 0, 1, 1, 1, 0, 0, 2)
SCATTER_KINDS = (1, 1, 1, 1, 2, 1, 0, 0, 1, 0, 0, 1, 0, 0)
GATHER_SWAPPED = (0, 1, 0, 1, 0, 0, 0, 0, 0, 0, 0, 0, 0)
SCATTER_SWAPPED = (0, 0, 0, 0, 0, 0, 0, 0, 0, 0, 1, 1, 0, 0)
GATHER, SCATTER, ROWS, SMALL, COMPUTE = range(5)
TOKENS, COTANGENT, BLOCK, GRADIENT = range(4)
(
    NORM_ONE,
    TURN_ONE,
    PROJECT,
    ATTEND,
    SEND_ONE,
    NORM_TWO,
    TURN_TWO,
    ACTIVATE,
    MASK,
    GRAD_DOWN,
    BACK_HIDDEN,
    GRAD_UP,
    SEND_TWO,
    OUTPUT,
    SEND_THREE,
    BACK_TWO,
    TURN_BACK,
    GRAD_OUT,
    BACK_CONTEXT,
    ATTEND_BACK,
    GRAD_IN,
    SEND_FOUR,
    BACK_ONE,
) = range(23)
SCHEDULE = (
    (GATHER, 3, 0),
    (ROWS, TOKENS, 0),
    (GATHER, 2, 0),
    (GATHER, 0, 0),
    (GATHER, 3, 1),
    (GATHER, 3, 2),
    (GATHER, 2, 1),
    (GATHER, 2, 2),
    (GATHER, 4, 0),
    (GATHER, 1, 0),
    (GATHER, 0, 1),
    (GATHER, 0, 2),
    (GATHER, 5, 0),
    (GATHER, 3, 3),
    (GATHER, 6, 0),
    (GATHER, 2, 3),
    (GATHER, 4, 1),
    (GATHER, 4, 2),
    (GATHER, 0, 3),
    (GATHER, 9, 0),
    (GATHER, 10, 0),
    (ROWS, TOKENS, 1),
    (GATHER, 1, 1),
    (GATHER, 1, 2),
    (GATHER, 1, 3),
    (GATHER, 2, 4),
    (GATHER, 6, 1),
    (GATHER, 9, 1),
    (GATHER, 12, 0),
    (GATHER, 5, 1),
    (GATHER, 3, 4),
    (ROWS, COTANGENT, 0),
    (ROWS, TOKENS, 2),
    (COMPUTE, NORM_ONE, 0),
    (COMPUTE, PROJECT, 2),
    (COMPUTE, PROJECT, 1),
    (GATHER, 11, 0),
    (GATHER, 4, 3),
    (GATHER, 6, 2),
    (COMPUTE, TURN_ONE, 0),
    (GATHER, 7, 0),
    (GATHER, 0, 4),
    (GATHER, 1, 4),
    (COMPUTE, PROJECT, 0),
    (COMPUTE, ATTEND, 0),
    (GATHER, 5, 2),
    (GATHER, 5, 3),
    (ROWS, COTANGENT, 1),
    (GATHER, 4, 4),
    (GATHER, 12, 1),
    (GATHER, 8, 0),
    (COMPUTE, ATTEND, 1),
    (GATHER, 11, 1),
    (GATHER, 11, 2),
    (GATHER, 9, 2),
    (GATHER, 9, 3),
    (COMPUTE, ATTEND, 3),
    (ROWS, COTANGENT, 2),
    (COMPUTE, MASK, 0),
    (GATHER, 10, 1),
    (GATHER, 10, 2),
    (GATHER, 7, 1),
    (GATHER, 8, 1),
    (COMPUTE, ATTEND, 2),
    (COMPUTE, SEND_ONE, 0),
    (COMPUTE, NORM_TWO, 0),
    (COMPUTE, TURN_TWO, 0),
    (GATHER, 8, 2),
    (GATHER, 6, 3),
    (GATHER, 10, 3),
    (GATHER, 7, 2),
    (GATHER, 7, 3),
    (GATHER, 12, 2),
    (GATHER, 12, 3),
    (GATHER, 11, 3),
    (GATHER, 8, 3),
    (GATHER, 5, 4),
    (COMPUTE, ACTIVATE, 0),
    (COMPUTE, GRAD_DOWN, 0),
    (SCATTER, 0, 0),
    (GATHER, 9, 4),
    (COMPUTE, BACK_HIDDEN, 0),
    (COMPUTE, GRAD_UP, 0),
    (SCATTER, 4, 0),
    (GATHER, 6, 4),
    (COMPUTE, ACTIVATE, 1),
    (COMPUTE, GRAD_DOWN, 1),
    (SCATTER, 1, 0),
    (GATHER, 7, 4),
    (COMPUTE, ACTIVATE, 2),
    (COMPUTE, GRAD_DOWN, 2),
    (SCATTER, 2, 0),
    (GATHER, 10, 4),
    (COMPUTE, BACK_HIDDEN, 1),
    (COMPUTE, GRAD_UP, 1),
    (SCATTER, 5, 0),
    (GATHER, 11, 4),
    (GATHER, 8, 4),
    (COMPUTE, ACTIVATE, 3),
    (COMPUTE, GRAD_DOWN, 3),
    (GATHER, 12, 4),
    (COMPUTE, SEND_TWO, 0),
    (COMPUTE, BACK_HIDDEN, 3),
    (COMPUTE, GRAD_UP, 3),
    (SCATTER, 7, 0),
    (SCATTER, 3, 0),
    (SCATTER, 1, 1),
    (COMPUTE, OUTPUT, 0),
    (COMPUTE, BACK_HIDDEN, 2),
    (COMPUTE, SEND_THREE, 0),
    (COMPUTE, GRAD_UP, 2),
    (SCATTER, 6, 0),
    (SCATTER, 0, 1),
    (SCATTER, 5, 1),
    (SCATTER, 4, 1),
    (SCATTER, 1, 2),
    (SCATTER, 2, 1),
    (COMPUTE, BACK_TWO, 0),
    (COMPUTE, BACK_CONTEXT, 0),
    (COMPUTE, ATTEND_BACK, 1),
    (COMPUTE, ATTEND_BACK, 2),
    (COMPUTE, TURN_BACK, 0),
    (SCATTER, 7, 1),
    (COMPUTE, GRAD_OUT, 0),
    (SCATTER, 8, 0),
    (SCATTER, 5, 2),
    (SCATTER, 0, 2),
    (COMPUTE, ATTEND_BACK, 0),
    (ROWS, BLOCK, 0),
    (SCATTER, 3, 1),
    (SCATTER, 7, 2),
    (COMPUTE, ATTEND_BACK, 3),
    (COMPUTE, GRAD_IN, 3),
    (SCATTER, 11, 0),
    (COMPUTE, GRAD_IN, 5),
    (SCATTER, 13, 0),
    (COMPUTE, SEND_FOUR, 0),
    (COMPUTE, GRAD_IN, 0),
    (COMPUTE, GRAD_IN, 4),
    (SCATTER, 12, 0),
    (COMPUTE, GRAD_IN, 1),
    (SCATTER, 9, 0),
    (SCATTER, 3, 2),
    (SCATTER, 11, 1),
    (SCATTER, 4, 2),
    (SCATTER, 6, 1),
    (SCATTER, 2, 2),
    (SCATTER, 8, 1),
    (COMPUTE, BACK_ONE, 0),
    (SMALL, 0, 0),
    (SMALL, 0, 1),
    (ROWS, GRADIENT, 0),
    (SCATTER, 6, 2),
    (SCATTER, 7, 3),
    (ROWS, BLOCK, 1),
    (SCATTER, 13, 1),
    (COMPUTE, GRAD_IN, 2),
    (SCATTER, 10, 0),
    (SMALL, 0, 2),
    (SCATTER, 10, 1),
    (SCATTER, 9, 1),
    (SCATTER, 8, 2),
    (SCATTER, 1, 3),
    (ROWS, GRADIENT, 1),
    (ROWS, GRADIENT, 2),
    (SCATTER, 13, 2),
    (SCATTER, 13, 3),
    (SCATTER, 5, 3),
    (SCATTER, 4, 3),
    (SCATTER, 11, 2),
    (SCATTER, 10, 2),
    (SCATTER, 10, 3),
    (SCATTER, 0, 3),
    (SCATTER, 12, 1),
    (SCATTER, 9, 2),
    (SCATTER, 3, 3),
    (SCATTER, 6, 3),
    (SCATTER, 8, 3),
    (SCATTER, 2, 3),
    (ROWS, BLOCK, 2),
    (SCATTER, 13, 4),
    (SCATTER, 0, 4),
    (SCATTER, 5, 4),
    (SMALL, 0, 3),
    (SCATTER, 1, 4),
    (SCATTER, 9, 3),
    (SCATTER, 11, 3),
    (SCATTER, 11, 4),
    (SCATTER, 12, 2),
    (SCATTER, 12, 3),
    (SCATTER, 10, 4),
    (SCATTER, 3, 4),
    (SCATTER, 2, 4),
    (SCATTER, 4, 4),
    (SCATTER, 7, 4),
    (SCATTER, 8, 4),
    (SCATTER, 9, 4),
    (SCATTER, 6, 4),
    (SCATTER, 12, 4),
)


def nn(left, right):
    return jnp.dot(left, right, preferred_element_type=F32)


def nt(left, right):
    return lax.dot_general(left, right, (((1,), (1,)), ((), ())), preferred_element_type=F32)


def loop(count, body, start=0):
    def step(index, carry):
        body(index)
        return carry

    lax.fori_loop(start, count, step, 0)


def part(index, size):
    return pl.ds(pl.multiple_of(index * size, size), size)


def fold(block):
    return jnp.sum(block.reshape(-1, 8, block.shape[-1]), axis=0)


def layer_kernel(
    chain,
    tokens,
    cotangent,
    segments,
    weight_in,
    weight_out,
    weight_up,
    weight_down,
    first_gain,
    first_shift,
    input_bias,
    output_bias,
    second_gain,
    second_shift,
    up_bias,
    block_out,
    token_grad,
    in_sum,
    out_sum,
    up_sum,
    down_sum,
    small_out,
    store,
    over,
    over_extra,
    row_in,
    row_up,
    plain,
    first_t,
    second_t,
    up_t,
    heads,
    context,
    context_grad,
    residual,
    slope,
    hidden,
    send,
    recv,
    score,
    other,
    prob_low,
    flip,
    turned,
    gather_acc,
    log_sums,
    sums,
    up_sums,
    head_sums,
    small,
    small_x,
    small_y,
    small_z,
    keep_col,
    keep_row,
    peaks,
    block_sum,
    gather_send,
    gather_recv,
    local_sem,
    scatter_send,
    scatter_recv,
    pair_send,
    pair_recv,
    row_send,
    row_recv,
    small_send,
    small_recv,
):
    place = lax.axis_index("fsdp")
    y = lax.axis_index("context")
    t = lax.axis_index("tensor")
    z = place // 2
    x = place % 2
    half = chain // 2
    mine = x * 2 + y
    at_ab = (1 - x) * 2 + (1 - y)
    to_x = {"fsdp": z * 2 + (1 - x)}
    to_y = {"context": 1 - y}
    to_t = {"tensor": 1 - t}

    def sides(swapped):
        if swapped:
            return x * 2 + (1 - y), (1 - x) * 2 + y, to_y, to_x
        a_x = x + (1 - t) * (1 - 2 * x)
        a_y = y + t * (1 - 2 * y)
        b_x = x + t * (1 - 2 * x)
        b_y = y + (1 - t) * (1 - 2 * y)
        to_a = {"fsdp": z * 2 + a_x, "context": a_y}
        to_b = {"fsdp": z * 2 + b_x, "context": b_y}
        return a_x * 2 + a_y, b_x * 2 + b_y, to_a, to_b

    normal_sides = sides(0)
    swapped_sides = sides(1)

    near = 1 - z + 4 * (z // 2)
    mate = 3 - z
    far = 3 - near
    inner = ((z + 1) // 2) % 2 == 1
    outer = ((z + 1) // 2) % 2 == 0

    def to_z(k):
        return {"fsdp": k * 2 + x}

    def remote(source, target, send_sem, recv_sem, device):
        return pltpu.make_async_remote_copy(
            src_ref=source,
            dst_ref=target,
            send_sem=send_sem,
            recv_sem=recv_sem,
            device_id=device,
            device_id_type=MESH_ID,
        )

    slots = row_in.shape[0]
    own_slots = slots // 2
    quarter = own_slots // 2
    width = row_in.shape[1]

    shards = (
        [weight_in.at[k] for k in range(3)]
        + [weight_out]
        + [weight_up.at[:, k * COLS : (k + 1) * COLS] for k in range(4)]
        + [weight_down.at[:, k * COLS : (k + 1) * COLS] for k in range(4)]
    )
    rows = weight_out.shape[0]

    def load(j):
        return pltpu.make_async_copy(shards[j], store.at[j + 8 * (j // 8), z, mine], local_sem.at[j])

    for j in range(PIECES):
        load(j).start()

    barrier = pltpu.get_barrier_semaphore()
    for device in [to_x, to_y, to_t] + [to_z((z + step) % chain) for step in range(1, chain)]:
        pl.semaphore_signal(barrier, inc=1, device_id=device, device_id_type=MESH_ID)
    pl.semaphore_wait(barrier, chain + 2)

    def gathered(j, at, quarter_at):
        piece, start, count = GATHER_PIECES[j]
        return store.at[piece + 8 * (piece // 8), at, quarter_at, :, start : start + count]

    def gather_way(j):
        return swapped_sides if GATHER_SWAPPED[j] else normal_sides

    def gather_z(j, stream, source, slot, target):
        if GATHER_KINDS[j] == 2:
            block = gathered(j, source, slice(None))
        else:
            block = gathered(j, source, gather_way(j)[0] if stream else mine)
        return remote(
            block,
            block,
            gather_send.at[j, 4 * stream + slot],
            gather_recv.at[j, 4 * stream + source],
            to_z(target),
        )

    def gather_start(j, stream):
        gather_z(j, stream, z, 0, near).start()
        gather_z(j, stream, z, 1, mate).start()

        @pl.when(outer)
        def _():
            gather_z(j, stream, z, 2, far).start()

    def gather_pass(j, stream):
        @pl.when(inner)
        def _():
            gather_z(j, stream, mate, 0, z).wait_recv()
            gather_z(j, stream, mate, 3, near).start()

    def gather_end(j, stream):
        gather_z(j, stream, near, 0, z).wait_recv()
        gather_z(j, stream, far, 0, z).wait_recv()
        gather_z(j, stream, z, 0, near).wait_send()
        gather_z(j, stream, z, 1, mate).wait_send()

        @pl.when(outer)
        def _():
            gather_z(j, stream, mate, 0, z).wait_recv()
            gather_z(j, stream, z, 2, far).wait_send()

        @pl.when(inner)
        def _():
            gather_z(j, stream, z, 3, near).wait_send()

    def gather_side(j, kind):
        at_a, _, to_a, to_b = gather_way(j)
        first = kind == 0 and GATHER_KINDS[j] == 1
        at = z if first or GATHER_KINDS[j] == 2 else slice(None)
        block = gathered(j, at, at_a if kind == 2 else mine)
        device = to_b if kind else to_a
        return remote(block, block, gather_send.at[j, 8 + kind], gather_recv.at[j, 8 + kind], device)

    def gather_stage(j, stage):
        piece = GATHER_PIECES[j][0]
        if piece not in loaded:
            load(piece).wait()
            loaded.add(piece)
        if GATHER_KINDS[j] == 2:
            if stage == 0:
                gather_side(j, 0).start()
                gather_side(j, 1).start()
            elif stage == 1:
                gather_side(j, 0).wait()
                gather_side(j, 2).start()
            elif stage == 2:
                gather_side(j, 1).wait()
                gather_side(j, 2).wait()
                gather_start(j, 0)
            elif stage == 3:
                gather_pass(j, 0)
            else:
                gather_end(j, 0)
        elif stage == 4:
            gather_side(j, 1).wait()
            gather_side(j, 2).wait()
        elif GATHER_KINDS[j]:
            if stage == 0:
                gather_side(j, 0).start()
                gather_start(j, 0)
            elif stage == 1:
                gather_side(j, 0).wait()
                gather_start(j, 1)
                gather_pass(j, 0)
            elif stage == 2:
                gather_pass(j, 1)
            else:
                gather_end(j, 0)
                gather_side(j, 1).start()
                gather_end(j, 1)
                gather_side(j, 2).start()
        elif stage == 0:
            gather_start(j, 0)
        elif stage == 1:
            gather_pass(j, 0)
        elif stage == 2:
            gather_end(j, 0)
            gather_side(j, 0).start()
            gather_side(j, 1).start()
        else:
            gather_side(j, 0).wait()
            gather_side(j, 2).start()

    def row_copies(source, target, which):
        mine_half = part(y, own_slots)
        local = pltpu.make_async_copy(source.at[y], target.at[mine_half], row_send.at[which, 2])
        place_there = pl.ds(pl.multiple_of(y * own_slots + t * quarter, quarter), quarter)
        across = remote(
            source.at[1 - y, part(t, quarter)],
            target.at[place_there],
            row_send.at[which, 0],
            row_recv.at[which, 0],
            to_y,
        )
        place_here = pl.ds(pl.multiple_of((1 - y) * own_slots + t * quarter, quarter), quarter)
        onward = remote(
            target.at[place_here], target.at[place_here], row_send.at[which, 1], row_recv.at[which, 1], to_t
        )
        return local, across, onward

    def row_back(source, target, which):
        mine_half = part(y, own_slots)
        local = pltpu.make_async_copy(source.at[mine_half], target.at[y], row_send.at[which, 2])
        from_here = pl.ds(pl.multiple_of((1 - y) * own_slots + t * quarter, quarter), quarter)
        across = remote(
            source.at[from_here],
            target.at[y, part(t, quarter)],
            row_send.at[which, 0],
            row_recv.at[which, 0],
            to_y,
        )
        block = target.at[1 - y, part(t, quarter)]
        onward = remote(block, block, row_send.at[which, 1], row_recv.at[which, 1], to_t)
        return local, across, onward

    token_local, token_across, token_on = row_copies(tokens, row_in, 0)
    up_local, up_across, up_on = row_copies(cotangent, row_up, 1)

    loaded = set()

    def stats(values):
        average = jnp.mean(values, axis=1, keepdims=True)
        centered = values - average
        inverse = lax.rsqrt(jnp.mean(centered * centered, axis=1, keepdims=True) + EPSILON)
        return centered * inverse, inverse

    norm_rows = 32

    def prepare():
        peaks[...] = jnp.full(peaks.shape, MASKED, F32)
        sums[...] = jnp.zeros(sums.shape, F32)
        keep_row[...] = jnp.where(segments[pl.ds(y, 1), :] > 0, 1.0, 0.0)
        keep_col[...] = jnp.broadcast_to(keep_row[...], (128, slots)).T

    def norm_first(i):
        at = part(i, norm_rows)
        scaled, _ = stats(row_in[at, :].astype(F32))
        plain[at, :] = (scaled * first_gain[...] + first_shift[...]).astype(BF)

    def turn(source, target):
        def body(j):
            target[part(j, 128), :] = source[:, part(j, 128)].T

        loop(width // 128, body)

    def project(c, which):
        at = part(c, TILE)
        tile = store[which, :, :, :, at].reshape(width, TILE)
        value = nn(plain[...], tile)
        if which != 1:
            value = value + input_bias[which // 2 : which // 2 + 1, at]
        heads[which, c] = value.astype(BF)

    lane = lax.broadcasted_iota(jnp.int32, (slots, 128), 1)
    chunk = 64
    n_chunks = slots // chunk

    def head_operands(pair, h):
        where_pair = part(pair % 2, 128)
        query = heads[0, pair // 2, :, where_pair].astype(F32) * (HEAD_DIM**-0.5)
        key = heads[1, pair // 2, :, where_pair].astype(F32)
        own = (lane < HEAD_DIM) if h == 0 else (lane >= HEAD_DIM)
        first = HEAD_DIM if h == 0 else 0
        flag = keep_col[:, 0:1]
        query = jnp.where(own, query, jnp.where(lane == first, flag, jnp.where(lane == first + 1, 1.0 - flag, 0.0)))
        key = jnp.where(
            lane == first, -BIG * (1.0 - flag), jnp.where(lane == first + 1, -BIG * flag, key)
        )
        return query.astype(BF), key.astype(BF), own

    def attend(pair):
        where_pair = part(pair % 2, 128)
        turned[...] = heads[2, pair // 2, :, where_pair].T
        for h in range(2):
            query, key, _ = head_operands(pair, h)
            score[...] = nt(key, query)

            def top(i, best):
                return jnp.maximum(best, jnp.max(score[part(i, chunk), :].reshape(-1, 8, slots), axis=0))

            best = lax.fori_loop(0, n_chunks, top, jnp.full((8, slots), -3e38, F32))
            highest = jnp.max(best, axis=0, keepdims=True)

            def power(i, total):
                at = part(i, chunk)
                powers = jnp.exp(score[at, :] - highest)
                prob_low[at, :] = powers.astype(BF)
                return total + fold(powers)

            total = lax.fori_loop(0, n_chunks, power, jnp.zeros((8, slots), F32))
            total = jnp.sum(total, axis=0, keepdims=True)
            mixed = nn(turned[h * HEAD_DIM : (h + 1) * HEAD_DIM, :], prob_low[...])
            flip[h * HEAD_DIM : (h + 1) * HEAD_DIM, :] = mixed / total
            log_sums[2 * pair + h] = highest + jnp.log(total)
            summit = jnp.max(jnp.where(keep_row[...] > 0.0, highest, MASKED), axis=1, keepdims=True)
            spots = lax.broadcasted_iota(jnp.int32, peaks.shape, 1)
            peaks[...] = jnp.where(spots == 2 * pair + h, summit, peaks[...])
        context[pair // 2, :, where_pair] = flip[...].T.astype(BF)

    def mask_rows(i):
        at = part(i, 64)
        row_up[at, :] = (row_up[at, :].astype(F32) * keep_col[at, 0:1]).astype(BF)

    def pair_copy(slot, j):
        return remote(send.at[j], recv.at[slot, j], pair_send.at[j], pair_recv.at[slot, j], to_t)

    def pair_sum(slot, product):
        def body(j):
            send[j] = product(j).astype(BF)
            pair_copy(slot, j).start()

        loop(4, body)

    def pair_wait(slot):
        for j in range(4):
            pair_copy(slot, j).wait()

    def summed(slot, at):
        return jnp.concatenate(
            [send[j, at, :].astype(F32) + recv[slot, j, at, :].astype(F32) for j in range(4)], axis=1
        )

    def weight_rows(piece, j, c):
        return store[piece, j, :, :, c * TILE : (c + 1) * TILE].reshape(TILE, TILE)

    def attended(j):
        return nt(context[0], weight_rows(3, j, 0)) + nt(context[1], weight_rows(3, j, 1))

    def norm_second(i):
        at = part(i, norm_rows)
        values = row_in[at, :].astype(F32) + summed(0, at) + output_bias[0:1, :]
        residual[at, :] = values
        scaled, _ = stats(values)
        plain[at, :] = (scaled * second_gain[...] + second_shift[...]).astype(BF)

    def activate(c):
        at = part(c % 2, TILE)
        tile = store[4 + c // 2, :, :, :, at].reshape(width, TILE)
        score[:, 0:TILE] = nn(plain[...], tile) + up_bias[0:1, part(c, TILE)]

        def rows_of(i):
            spot = part(i, 64)
            pre = score[spot, 0:TILE]
            chance = 0.5 * (1.0 + lax.erf(pre * HALF_ROOT))
            hidden[c, spot, :] = (pre * chance).astype(BF)
            slope[c, spot, :] = (chance + pre * jnp.exp(-0.5 * pre * pre) * DENSITY).astype(BF)

        loop(slots // 64, rows_of)

    def z_spot(p, stream, spot):
        return (stream if SCATTER_KINDS[p] else 1) * chain + spot

    def columns(p):
        _, start, count = SCATTER_PIECES[p]
        return slice(start, start + count)

    def scatter_way(p):
        return swapped_sides if SCATTER_SWAPPED[p] else normal_sides

    def partial(p, at, quarter_at):
        return store.at[8 + SCATTER_PIECES[p][0], at, quarter_at, :, columns(p)]

    def from_b(p, which, at):
        if SCATTER_KINDS[p] == 2:
            return over_extra.at[which, :, columns(p)]
        if at is None:
            return over.at[SCATTER_PIECES[p][0], which * chain : (which + 1) * chain, :, columns(p)]
        return over.at[SCATTER_PIECES[p][0], which * chain + at, :, columns(p)]

    def from_rest(p, at):
        if at is None:
            return over.at[SCATTER_PIECES[p][0], 2 * chain : 3 * chain, :, columns(p)]
        return over.at[SCATTER_PIECES[p][0], 2 * chain + at, :, columns(p)]

    def scatter_side(p, kind):
        at_a, at_b, to_a, to_b = scatter_way(p)
        sems = (scatter_send.at[p, kind], scatter_recv.at[p, kind])
        at = z if SCATTER_KINDS[p] == 2 else slice(None)
        if kind < 2:
            return remote(partial(p, at, at_ab if kind else at_b), from_b(p, kind, None), *sems, to_b)
        if SCATTER_KINDS[p]:
            return remote(partial(p, z, at_a), from_rest(p, 2 * chain), *sems, to_a)
        return remote(partial(p, at, at_a), from_rest(p, None), *sems, to_a)

    def own_quarter(p, stream):
        if SCATTER_KINDS[p] == 2:
            return slice(None)
        return scatter_way(p)[0] if stream else mine

    def from_z(p, stream, spot):
        if SCATTER_KINDS[p] == 2:
            return over.at[SCATTER_PIECES[p][0], pl.ds(4 * spot, 4), :, columns(p)]
        return from_rest(p, z_spot(p, stream, spot))

    def scatter_z(p, stream, slot, block, spot, target):
        return remote(
            partial(p, block, own_quarter(p, stream)),
            from_z(p, stream, spot),
            scatter_send.at[p, 3 + 4 * stream + slot],
            scatter_recv.at[p, 3 + 4 * stream + spot],
            to_z(target),
        )

    def add_to(ref, *terms):
        total = ref[...].astype(F32)
        for term in terms:
            total = total + term[...].astype(F32)
        ref[...] = total.astype(BF)

    def scatter_start(p, stream):
        scatter_z(p, stream, 0, near, z, near).start()

        @pl.when(outer)
        def _():
            scatter_z(p, stream, 1, mate, z, mate).start()
            scatter_z(p, stream, 2, far, near, near).start()

        @pl.when(inner)
        def _():
            scatter_z(p, stream, 2, far, z, far).start()

    def scatter_pass(p, stream):
        @pl.when(inner)
        def _():
            scatter_z(p, stream, 0, near, z, near).wait_recv()
            add_to(partial(p, mate, own_quarter(p, stream)), from_z(p, stream, z))
            scatter_z(p, stream, 1, mate, z, mate).start()

    def scatter_end(p, stream):
        scatter_z(p, stream, 0, near, near, near).wait_recv()
        scatter_z(p, stream, 0, near, mate, near).wait_recv()
        scatter_z(p, stream, 0, near, z, near).wait_send()
        scatter_z(p, stream, 1, mate, z, mate).wait_send()
        if SCATTER_KINDS[p] == 2:
            add_to(partial(p, z, slice(None)), from_z(p, stream, near), from_z(p, stream, mate))
        else:
            block_sum[:, columns(p)] = (
                partial(p, z, own_quarter(p, stream))[...].astype(F32)
                + from_z(p, stream, near)[...].astype(F32)
                + from_z(p, stream, mate)[...].astype(F32)
            )

        @pl.when(outer)
        def _():
            scatter_z(p, stream, 0, near, far, near).wait_recv()
            if SCATTER_KINDS[p] == 2:
                add_to(partial(p, z, slice(None)), from_z(p, stream, far))
            else:
                block_sum[:, columns(p)] += from_z(p, stream, far)[...].astype(F32)

        scatter_z(p, stream, 2, far, z, far).wait_send()

    def scatter_target(p):
        piece, start, count = SCATTER_PIECES[p]
        if piece < 4:
            return down_sum.at[:, piece * COLS + start : piece * COLS + start + count]
        if piece < 8:
            return up_sum.at[:, (piece - 4) * COLS + start : (piece - 4) * COLS + start + count]
        if piece == 8:
            return out_sum.at[:, start : start + count]
        return in_sum.at[piece - 9, :, start : start + count]

    def scatter_stage(p, stage):
        late = SCATTER_KINDS[p]
        at_a = scatter_way(p)[0]
        if late == 2:
            if stage == 0:
                scatter_start(p, 0)
            elif stage == 1:
                scatter_pass(p, 0)
            elif stage == 2:
                scatter_end(p, 0)
                scatter_side(p, 0).start()
                scatter_side(p, 1).start()
            elif stage == 3:
                scatter_side(p, 0).wait()
                scatter_side(p, 1).wait()
                add_to(partial(p, z, mine), from_b(p, 0, None))
                add_to(partial(p, z, at_a), from_b(p, 1, None))
                scatter_side(p, 2).start()
            else:
                scatter_side(p, 2).wait()
                last = partial(p, z, mine)[...].astype(F32)
                scatter_target(p)[...] = last + from_rest(p, 2 * chain)[...].astype(F32)
        elif stage == 0:
            scatter_side(p, 0).start()
            scatter_side(p, 1).start()
        elif stage == 1:
            scatter_side(p, 0).wait()
            scatter_side(p, 1).wait()

            def body(k):
                add_to(partial(p, k, mine), from_b(p, 0, k))
                add_to(partial(p, k, at_a), from_b(p, 1, k))

            loop(chain, body)
            if late:
                scatter_start(p, 0)
                scatter_start(p, 1)
            else:
                scatter_side(p, 2).start()
        elif stage == 2:
            if late:
                scatter_pass(p, 0)
                scatter_pass(p, 1)
            else:
                scatter_side(p, 2).wait()
                loop(chain, lambda k: add_to(partial(p, k, mine), from_rest(p, k)))
                scatter_start(p, 0)
        elif stage == 3:
            if late:
                scatter_end(p, 1)
                partial(p, z, at_a)[...] = block_sum[:, columns(p)].astype(BF)
                scatter_side(p, 2).start()
            else:
                scatter_pass(p, 0)
        else:
            scatter_end(p, 0)
            total = block_sum[:, columns(p)]
            if late:
                scatter_side(p, 2).wait()
                total = total + from_rest(p, 2 * chain)[...].astype(F32)
            scatter_target(p)[...] = total

    def gradient(left, right, piece, c):
        def body(m):
            block = nn(left[part(m, width // 2), :], right)
            store[8 + piece, part(m, half), :, :, part(c, TILE)] = block.astype(BF).reshape(half, 4, rows, TILE)

        loop(2, body)

    def back_hidden(c):
        at = part(c % 2, TILE)
        tile = store[16 + c // 2, :, :, :, at].reshape(width, TILE)
        score[:, 0:TILE] = nn(row_up[...], tile)

        def rows_of(i, total):
            spot = part(i, 64)
            grad = (score[spot, 0:TILE] * slope[c, spot, :].astype(F32)).astype(BF)
            slope[c, spot, :] = grad
            return total + fold(grad.astype(F32))

        total = lax.fori_loop(0, slots // 64, rows_of, jnp.zeros((8, TILE), F32))
        up_sums[c] = jnp.sum(total, axis=0, keepdims=True)

    def mixed(j):
        total = nt(hidden[0], weight_rows(16, j, 0))
        for c in range(1, 8):
            total = total + nt(hidden[c], weight_rows(16 + c // 2, j, c % 2))
        return total

    def output_rows(i):
        at = part(i, norm_rows)
        values = residual[at, :] + summed(1, at) + output_bias[1:2, :]
        plain[at, :] = (values * keep_col[at, 0:1]).astype(BF)

    block_local, block_across, block_on = row_back(plain, block_out, 2)

    def second_back(j):
        total = nt(slope[0], weight_rows(4, j, 0))
        for c in range(1, 8):
            total = total + nt(slope[c], weight_rows(4 + c // 2, j, c % 2))
        return total

    def norm_second_back(i):
        at = part(i, norm_rows)
        scaled, inverse = stats(residual[at, :])
        incoming = summed(0, at)
        weighted = incoming * second_gain[...]
        upstream = row_up[at, :].astype(F32)
        bracket = (
            weighted
            - jnp.mean(weighted, axis=1, keepdims=True)
            - scaled * jnp.mean(weighted * scaled, axis=1, keepdims=True)
        )
        total = upstream + inverse * bracket
        residual[at, :] = total
        low = total.astype(BF)
        for j in range(4):
            hidden[4 + j, at, :] = low[:, j * TILE : (j + 1) * TILE]
        sums[0] += fold(incoming * scaled)
        sums[1] += fold(incoming)
        sums[2] += fold(total)
        sums[3] += fold(upstream)

    def turn_attend():
        for j in range(4):
            for k in range(2):
                at = j * TILE + k * 128
                up_t[at : at + 128, :] = hidden[4 + j, :, k * 128 : (k + 1) * 128].T

    def back_context(c):
        total = None
        for j in range(4):
            tile = store[3, j, :, :, part(c, TILE)].reshape(TILE, TILE)
            term = nn(hidden[4 + j], tile)
            total = term if total is None else total + term
        context_grad[c] = total.astype(BF)

    def attend_back(pair):
        where_pair = part(pair % 2, 128)
        turned[...] = heads[1, pair // 2, :, where_pair].T
        value = heads[2, pair // 2, :, where_pair]
        incoming = context_grad[pair // 2, :, where_pair]
        for h in range(2):
            query, key, own = head_operands(pair, h)
            own_in = jnp.where(own, incoming.astype(F32), 0.0).astype(BF)
            score[...] = nt(key, query)
            other[...] = nt(value, own_in)
            logs = log_sums[2 * pair + h]

            def power(i, total):
                at = part(i, chunk)
                probs = jnp.exp(score[at, :] - logs)
                score[at, :] = probs
                prob_low[at, :] = probs.astype(BF)
                return total + fold(probs * other[at, :])

            total = lax.fori_loop(0, n_chunks, power, jnp.zeros((8, slots), F32))
            centre = jnp.sum(total, axis=0, keepdims=True)

            value_grad = nn(prob_low[...], own_in)

            def rest(i):
                at = part(i, chunk)
                prob_low[at, :] = (score[at, :] * (other[at, :] - centre)).astype(BF)

            loop(n_chunks, rest)
            key_grad = nn(prob_low[...], query)
            if h == 0:
                gather_acc[0] = value_grad.astype(BF)
                gather_acc[1] = key_grad.astype(BF)
            else:
                gather_acc[0] = jnp.where(own, value_grad, gather_acc[0].astype(F32)).astype(BF)
                gather_acc[1] = jnp.where(own, key_grad, gather_acc[1].astype(F32)).astype(BF)
            flip[h * HEAD_DIM : (h + 1) * HEAD_DIM, :] = nn(
                turned[h * HEAD_DIM : (h + 1) * HEAD_DIM, :], prob_low[...]
            ) * (HEAD_DIM**-0.5)
        query_low = flip[...].T.astype(BF)
        value_low = gather_acc[0]
        heads[0, pair // 2, :, where_pair] = query_low
        heads[1, pair // 2, :, where_pair] = gather_acc[1]
        heads[2, pair // 2, :, where_pair] = value_low
        head_sums[0, pair] = jnp.sum(query_low.astype(F32), axis=0, keepdims=True)
        head_sums[1, pair] = jnp.sum(value_low.astype(F32), axis=0, keepdims=True)

    def first_back(j):
        total = None
        for i in range(3):
            for c in range(2):
                term = nt(heads[i, c], weight_rows(i, j, c))
                total = term if total is None else total + term
        return total

    def norm_first_back(i):
        at = part(i, norm_rows)
        scaled, inverse = stats(row_in[at, :].astype(F32))
        incoming = summed(1, at)
        weighted = incoming * first_gain[...]
        bracket = (
            weighted
            - jnp.mean(weighted, axis=1, keepdims=True)
            - scaled * jnp.mean(weighted * scaled, axis=1, keepdims=True)
        )
        row_in[at, :] = (residual[at, :] + inverse * bracket).astype(BF)
        sums[4] += fold(incoming * scaled)
        sums[5] += fold(incoming)

    grad_local, grad_across, grad_on = row_back(row_in, token_grad, 3)

    def collapse(k):
        return jnp.sum(sums[k], axis=0, keepdims=True)

    def small_fill():
        small[0:1, :] = collapse(4)
        small[1:2, :] = collapse(5)
        small[2:3, :] = jnp.concatenate([head_sums[i, k] for i in range(2) for k in range(4)], axis=1)
        small[3:4, :] = collapse(2)
        small[4:5, :] = collapse(3)
        small[5:6, :] = collapse(0)
        small[6:7, :] = collapse(1)
        small[7:8, :] = jnp.concatenate([up_sums[k] for k in range(4)], axis=1)
        small[8:9, :] = jnp.concatenate([up_sums[4 + k] for k in range(4)], axis=1)
        small[9:10, :] = jnp.concatenate([peaks[0:1, :]] * 8, axis=1)
        small[10:16, :] = jnp.zeros((6, small.shape[1]), F32)

    row_index = lax.broadcasted_iota(jnp.int32, small.shape, 0)

    def joined(left, right):
        return jnp.where(row_index == 9, jnp.maximum(left, right), left + right)

    def small_copy(source, target, k, device):
        return remote(source, target, small_send.at[k], small_recv.at[k], device)

    over_x = small_copy(small, small_x.at[0], 0, to_x)
    over_y = small_copy(small_x.at[1], small_y, 1, to_y)
    along_z = [
        small_copy(small_z.at[z], small_z.at[z], 1 + step, to_z((z + step) % chain)) for step in range(1, chain)
    ]

    def small_stage(stage):
        if stage == 0:
            small_fill()
            over_x.start()
        elif stage == 1:
            over_x.wait()
            small_x[1] = joined(small[...], small_x[0])
            over_y.start()
        elif stage == 2:
            over_y.wait()
            small_z[z] = joined(small_x[1], small_y[...])
            for copy in along_z:
                copy.start()
        else:
            for copy in along_z:
                copy.wait()
            total = small_z[0]
            for k in range(1, chain):
                total = joined(total, small_z[k])
            small_out[...] = total

    rows_over = {
        TOKENS: (token_local, token_across, token_on),
        COTANGENT: (up_local, up_across, up_on),
        BLOCK: (block_local, block_across, block_on),
        GRADIENT: (grad_local, grad_across, grad_on),
    }

    def rows_stage(which, stage):
        local, across, onward = rows_over[which]
        if stage == 0:
            local.start()
            across.start()
        elif stage == 1:
            across.wait()
            onward.start()
        else:
            onward.wait()
            local.wait()

    def norms(slot, body):
        pair_wait(slot)
        loop(slots // norm_rows, body)

    def mask_and_turn():
        loop(slots // 64, mask_rows)
        turn(row_up, up_t)

    compute = {
        NORM_ONE: lambda i: (prepare(), loop(slots // norm_rows, norm_first)),
        TURN_ONE: lambda i: turn(plain, first_t),
        PROJECT: lambda i: loop(2, lambda c: project(c, i)),
        ATTEND: attend,
        SEND_ONE: lambda i: pair_sum(0, attended),
        NORM_TWO: lambda i: norms(0, norm_second),
        TURN_TWO: lambda i: turn(plain, second_t),
        ACTIVATE: lambda i: loop(2 * i + 2, activate, 2 * i),
        MASK: lambda i: mask_and_turn(),
        GRAD_DOWN: lambda i: loop(2, lambda c: gradient(up_t, hidden[2 * i + c], i, c)),
        BACK_HIDDEN: lambda i: loop(2 * i + 2, back_hidden, 2 * i),
        GRAD_UP: lambda i: loop(2, lambda c: gradient(second_t, slope[2 * i + c], 4 + i, c)),
        SEND_TWO: lambda i: pair_sum(1, mixed),
        OUTPUT: lambda i: norms(1, output_rows),
        SEND_THREE: lambda i: pair_sum(0, second_back),
        BACK_TWO: lambda i: norms(0, norm_second_back),
        TURN_BACK: lambda i: turn_attend(),
        GRAD_OUT: lambda i: loop(2, lambda c: gradient(up_t, context[c], 8, c)),
        BACK_CONTEXT: lambda i: loop(2, back_context),
        ATTEND_BACK: attend_back,
        GRAD_IN: lambda i: gradient(first_t, heads[i // 2, i % 2], 9 + i // 2, i % 2),
        SEND_FOUR: lambda i: pair_sum(1, first_back),
        BACK_ONE: lambda i: norms(1, norm_first_back),
    }
    for kind, which, index in SCHEDULE:
        if kind == GATHER:
            gather_stage(which, index)
        elif kind == SCATTER:
            scatter_stage(which, index)
        elif kind == ROWS:
            rows_stage(which, index)
        elif kind == SMALL:
            small_stage(index)
        else:
            compute[which](index)


def finish_kernel(
    block_in,
    grad_in,
    in_sum,
    out_sum,
    up_sum,
    down_sum,
    small,
    weight,
    block_out,
    grad_out,
    first_gain,
    first_shift,
    in_out,
    in_bias,
    out_out,
    out_bias,
    second_gain,
    second_shift,
    up_out,
    up_bias,
    down_out,
    clipped,
    factor,
):
    block_out[...] = block_in[...]
    grad_out[...] = grad_in[...].astype(F32)
    out_out[...] = out_sum[...]
    up_out[...] = up_sum[...]
    down_out[...] = down_sum[...]
    local = out_sum.shape[1]
    in_out[...] = in_sum[...]
    first_gain[...] = small[0, :]
    first_shift[...] = small[1, :]
    in_bias[0:1, :] = small[2:3, 0:local]
    in_bias[1:2, :] = small[2:3, local:]
    out_bias[...] = small[3:5, :]
    second_gain[...] = small[5, :]
    second_shift[...] = small[6, :]
    width = small.shape[1]
    up_bias[0:width] = small[7, :]
    up_bias[width:] = small[8, :]
    factors = CLIP_LIMIT / jnp.maximum(small[9:10, 0:128], CLIP_LIMIT)
    factor[...] = factors[0, 0 : factor.shape[0]]
    roots = jnp.sqrt(factors)
    head = lax.broadcasted_iota(jnp.int32, (1, local), 1) // HEAD_DIM
    scale = jnp.zeros((1, local), F32)
    for h in range(local // HEAD_DIM):
        scale = jnp.where(head == h, roots[:, h : h + 1], scale)
    for k in range(2):
        clipped[:, k, :] = weight[k].astype(F32) * scale


def on_device_fused(
    tokens,
    segments,
    first_gain,
    first_shift,
    input_weight,
    input_bias,
    output_weight,
    output_bias,
    second_gain,
    second_shift,
    up_weight,
    up_bias,
    down_weight,
    cotangent,
    chain,
):
    group, tok_rows, width = tokens.shape
    slots = segments.shape[1]
    rows = input_weight.shape[0]
    weights = jnp.transpose(input_weight, (1, 0, 2))
    operands = (
        tokens,
        cotangent,
        segments,
        weights,
        output_weight,
        up_weight,
        down_weight,
        first_gain[None],
        first_shift[None],
        input_bias,
        output_bias,
        second_gain[None],
        second_shift[None],
        up_bias[None],
    )
    anywhere = pl.BlockSpec(memory_space=pl.ANY)
    vmem = pl.BlockSpec(memory_space=pltpu.VMEM)
    block = (rows, COLS)
    dma = pltpu.SemaphoreType.DMA
    results = pl.pallas_call(
        functools.partial(layer_kernel, chain),
        out_shape=(
            jax.ShapeDtypeStruct(tokens.shape, BF),
            jax.ShapeDtypeStruct(tokens.shape, BF),
            jax.ShapeDtypeStruct((3, rows, COLS), F32),
            jax.ShapeDtypeStruct((rows, COLS), F32),
            jax.ShapeDtypeStruct((rows, 4 * COLS), F32),
            jax.ShapeDtypeStruct((rows, 4 * COLS), F32),
            jax.ShapeDtypeStruct((16, width), F32),
        ),
        in_specs=[anywhere] * 2 + [vmem] + [anywhere] * 4 + [vmem] * 7,
        out_specs=[anywhere] * 2 + [vmem] * 5,
        scratch_shapes=[
            pltpu.VMEM((20, chain, 4) + block, BF),
            pltpu.VMEM((PIECES, 4 * chain + 1) + block, BF),
            pltpu.VMEM((2,) + block, BF),
            pltpu.VMEM((slots, width), BF),
            pltpu.VMEM((slots, width), BF),
            pltpu.VMEM((slots, width), BF),
            pltpu.VMEM((width, slots), BF),
            pltpu.VMEM((width, slots), BF),
            pltpu.VMEM((width, slots), BF),
            pltpu.VMEM((3, 2, slots, TILE), BF),
            pltpu.VMEM((2, slots, TILE), BF),
            pltpu.VMEM((2, slots, TILE), BF),
            pltpu.VMEM((slots, width), F32),
            pltpu.VMEM((8, slots, TILE), BF),
            pltpu.VMEM((8, slots, TILE), BF),
            pltpu.VMEM((4, slots, TILE), BF),
            pltpu.VMEM((2, 4, slots, TILE), BF),
            pltpu.VMEM((slots, slots), F32),
            pltpu.VMEM((slots, slots), F32),
            pltpu.VMEM((slots, slots), BF),
            pltpu.VMEM((128, slots), F32),
            pltpu.VMEM((128, slots), BF),
            pltpu.VMEM((2, slots, 128), BF),
            pltpu.VMEM((8, 1, slots), F32),
            pltpu.VMEM((6, 8, width), F32),
            pltpu.VMEM((8, 1, TILE), F32),
            pltpu.VMEM((2, 4, 1, 128), F32),
            pltpu.VMEM((16, width), F32),
            pltpu.VMEM((2, 16, width), F32),
            pltpu.VMEM((16, width), F32),
            pltpu.VMEM((chain, 16, width), F32),
            pltpu.VMEM((slots, 128), F32),
            pltpu.VMEM((1, slots), F32),
            pltpu.VMEM((8, 128), F32),
            pltpu.VMEM(block, F32),
            dma((len(GATHER_PIECES), 11)),
            dma((len(GATHER_PIECES), 11)),
            dma((PIECES,)),
            dma((len(SCATTER_PIECES), 11)),
            dma((len(SCATTER_PIECES), 11)),
            dma((4,)),
            dma((2, 4)),
            dma((4, 3)),
            dma((4, 2)),
            dma((2 + chain,)),
            dma((2 + chain,)),
        ],
        compiler_params=pltpu.CompilerParams(
            collective_id=0, has_side_effects=True, vmem_limit_bytes=67043328
        ),
        name="layer",
    )(*operands)
    local = input_weight.shape[2]
    flat = jax.ShapeDtypeStruct((width,), F32)
    finished = pl.pallas_call(
        finish_kernel,
        out_shape=(
            jax.ShapeDtypeStruct(tokens.shape, BF),
            jax.ShapeDtypeStruct(tokens.shape, F32),
            flat,
            flat,
            jax.ShapeDtypeStruct(weights.shape, F32),
            jax.ShapeDtypeStruct(input_bias.shape, F32),
            jax.ShapeDtypeStruct((rows, local), F32),
            jax.ShapeDtypeStruct(output_bias.shape, F32),
            flat,
            flat,
            jax.ShapeDtypeStruct(up_weight.shape, F32),
            jax.ShapeDtypeStruct(up_bias.shape, F32),
            jax.ShapeDtypeStruct(down_weight.shape, F32),
            jax.ShapeDtypeStruct((rows, 2, local), F32),
            jax.ShapeDtypeStruct((local // HEAD_DIM,), F32),
        ),
        in_specs=[vmem] * 8,
        out_specs=[vmem] * 15,
        name="finish",
    )(*results, weights)
    return finished[:4] + (jnp.transpose(finished[4], (1, 0, 2)),) + finished[5:]


def on_device(
    tokens,
    segments,
    first_gain,
    first_shift,
    input_weight,
    input_bias,
    output_weight,
    output_bias,
    second_gain,
    second_shift,
    up_weight,
    up_bias,
    down_weight,
    cotangent,
):
    group = tokens.shape[0]
    tok_rows = tokens.shape[1]
    width = tokens.shape[2]
    score_scale = HEAD_DIM ** (-0.5)
    position = lax.axis_index("context") * tok_rows
    query_segments = lax.dynamic_slice_in_dim(segments, position, tok_rows, 1)
    allowed = segments[:, None, :] == query_segments[:, :, None]
    real_pairs = allowed & (query_segments[:, :, None] > 0)
    keep_rows = (query_segments > 0).astype(jnp.float32).reshape(-1)[:, None]
    input_full, output_full = (
        lax.all_gather(input_weight, ("fsdp", "context"), axis=0, tiled=True),
        lax.all_gather(output_weight, ("fsdp", "context"), axis=0, tiled=True),
    )
    tokens_float = tokens.astype(jnp.float32).reshape(group * tok_rows, width)
    normed_one, scaled_one, inverse_one = normalize(tokens_float, first_gain, first_shift)
    first_operand = normed_one.astype(jnp.bfloat16)
    projected = jnp.einsum(
        "td,dcf->tcf", first_operand, input_full, preferred_element_type=jnp.float32
    )
    bias_rows = jnp.stack([input_bias[0], jnp.zeros_like(input_bias[0]), input_bias[1]])
    projected = (projected + bias_rows[None]).astype(jnp.bfloat16)
    local_width = projected.shape[2]
    projected = projected.reshape(group, tok_rows, 3, local_width)
    sources = lax.all_gather(projected[:, :, 1:], "context", axis=1, tiled=True)
    query_heads = split_heads(projected[:, :, 0])
    key_heads = split_heads(sources[:, :, 0])
    value_heads = split_heads(sources[:, :, 1])

    def head_forward(operands):
        query_one, key_one, value_one = operands
        logits = (
            jnp.einsum("gqd,gkd->gqk", query_one, key_one, preferred_element_type=jnp.float32)
            * score_scale
        )
        masked = jnp.where(allowed, logits, MASKED)
        summit = jnp.max(jnp.where(real_pairs, logits, MASKED))
        highest = jnp.max(masked, axis=2, keepdims=True)
        powers = jnp.exp(masked - highest)
        totals = jnp.sum(powers, axis=2, keepdims=True)
        weights_low = (powers / totals).astype(jnp.bfloat16)
        mixed = jnp.einsum(
            "gqk,gkd->gqd", weights_low, value_one, preferred_element_type=jnp.float32
        )
        return (mixed.astype(jnp.bfloat16), (highest + jnp.log(totals))[:, :, 0], summit)

    head_context, log_totals, summits = lax.map(head_forward, (query_heads, key_heads, value_heads))
    context = join_heads(head_context).reshape(group * tok_rows, local_width)
    attended = lax.psum(
        jnp.einsum("tf,df->td", context, output_full, preferred_element_type=jnp.float32), "tensor"
    )
    residual = tokens_float + attended + output_bias[0]
    peaks = lax.pmax(summits, ("fsdp", "context"))
    up_full, down_full = (
        lax.all_gather(up_weight, ("fsdp", "context"), axis=0, tiled=True),
        lax.all_gather(down_weight, ("fsdp", "context"), axis=0, tiled=True),
    )
    normed_two, scaled_two, inverse_two = normalize(residual, second_gain, second_shift)
    second_operand = normed_two.astype(jnp.bfloat16)
    pre_act = jnp.dot(second_operand, up_full, preferred_element_type=jnp.float32) + up_bias
    hidden = jax.nn.gelu(pre_act, approximate=False).astype(jnp.bfloat16)
    mixed_sum = lax.psum(
        jnp.einsum("tf,df->td", hidden, down_full, preferred_element_type=jnp.float32).astype(
            jnp.bfloat16
        ),
        "tensor",
    ).astype(jnp.float32)
    block_output = ((residual + mixed_sum + output_bias[1]) * keep_rows).astype(jnp.bfloat16)
    factor = CLIP_LIMIT / jnp.maximum(peaks, CLIP_LIMIT)
    column_scale = jnp.repeat(jnp.sqrt(factor), HEAD_DIM)
    clipped_weight = input_weight[:, :2, :].astype(jnp.float32) * column_scale[None, None, :]
    input_full, output_full, up_full, down_full = (
        lax.all_gather(input_weight, ("fsdp", "context"), axis=0, tiled=True),
        lax.all_gather(output_weight, ("fsdp", "context"), axis=0, tiled=True),
        lax.all_gather(up_weight, ("fsdp", "context"), axis=0, tiled=True),
        lax.all_gather(down_weight, ("fsdp", "context"), axis=0, tiled=True),
    )
    upstream = cotangent.astype(jnp.float32).reshape(group * tok_rows, width) * keep_rows
    upstream_low = upstream.astype(jnp.bfloat16)
    down_gradient = jnp.einsum(
        "td,tf->df", upstream_low, hidden, preferred_element_type=jnp.float32
    )
    pre_gradient = (
        jnp.dot(upstream_low, down_full, preferred_element_type=jnp.float32) * gelu_slope(pre_act)
    ).astype(jnp.bfloat16)
    up_gradient = jnp.einsum(
        "td,tf->df", second_operand, pre_gradient, preferred_element_type=jnp.float32
    )
    up_bias_gradient = jnp.sum(pre_gradient.astype(jnp.float32), axis=0)
    second_gradient = lax.psum(
        jnp.einsum("tf,df->td", pre_gradient, up_full, preferred_element_type=jnp.float32), "tensor"
    )
    through_two, second_gain_gradient, second_shift_gradient = normalize_back(
        second_gradient, scaled_two, inverse_two, second_gain
    )
    residual_gradient = upstream + through_two
    output_bias_gradient = jnp.stack(
        [jnp.sum(residual_gradient, axis=0), jnp.sum(upstream, axis=0)]
    )
    attend_low = residual_gradient.astype(jnp.bfloat16)
    output_gradient = jnp.einsum(
        "td,tf->df", attend_low, context, preferred_element_type=jnp.float32
    )
    context_back = jnp.dot(attend_low, output_full, preferred_element_type=jnp.float32).astype(
        jnp.bfloat16
    )
    context_gradient = split_heads(context_back.reshape(group, tok_rows, local_width))

    def head_backward(operands):
        query_one, key_one, value_one, incoming, log_total = operands
        logits = (
            jnp.einsum("gqd,gkd->gqk", query_one, key_one, preferred_element_type=jnp.float32)
            * score_scale
        )
        probs = jnp.exp(jnp.where(allowed, logits, MASKED) - log_total[:, :, None])
        prob_gradient = jnp.einsum(
            "gqd,gkd->gqk", incoming, value_one, preferred_element_type=jnp.float32
        )
        centre = jnp.sum(probs * prob_gradient, axis=2, keepdims=True)
        score_low = (probs * (prob_gradient - centre) * score_scale).astype(jnp.bfloat16)
        query_gradient = jnp.einsum(
            "gqk,gkd->gqd", score_low, key_one, preferred_element_type=jnp.float32
        ).astype(jnp.bfloat16)
        key_gradient = jnp.einsum(
            "gqk,gqd->gkd", score_low, query_one, preferred_element_type=jnp.float32
        )
        value_gradient = jnp.einsum(
            "gqk,gqd->gkd", probs.astype(jnp.bfloat16), incoming, preferred_element_type=jnp.float32
        )
        return (query_gradient, key_gradient, value_gradient)

    query_grads, key_grads, value_grads = lax.map(
        head_backward, (query_heads, key_heads, value_heads, context_gradient, log_totals)
    )
    source_terms = jnp.stack([join_heads(key_grads), join_heads(value_grads)], axis=2)
    source_sums = lax.psum_scatter(
        source_terms.astype(jnp.bfloat16), "context", scatter_dimension=1, tiled=True
    )
    source_low = source_sums.reshape(group * tok_rows, 2, local_width)
    query_flat = join_heads(query_grads).reshape(group * tok_rows, local_width)
    projected_gradient = jnp.concatenate([query_flat[:, None, :], source_low], axis=1)
    input_gradient = jnp.einsum(
        "td,tcf->dcf", first_operand, projected_gradient, preferred_element_type=jnp.float32
    )
    input_bias_gradient = jnp.stack(
        [
            jnp.sum(projected_gradient[:, 0].astype(jnp.float32), axis=0),
            jnp.sum(projected_gradient[:, 2].astype(jnp.float32), axis=0),
        ]
    )
    first_gradient = lax.psum(
        jnp.einsum(
            "tcf,dcf->td", projected_gradient, input_full, preferred_element_type=jnp.float32
        ).astype(jnp.bfloat16),
        "tensor",
    ).astype(jnp.float32)
    through_one, first_gain_gradient, first_shift_gradient = normalize_back(
        first_gradient, scaled_one, inverse_one, first_gain
    )
    tokens_gradient = (residual_gradient + through_one).reshape(group, tok_rows, width)
    block_output = block_output.reshape(group, tok_rows, width)
    (
        first_gain_sum,
        first_shift_sum,
        input_bias_sum,
        output_bias_sum,
        second_gain_sum,
        second_shift_sum,
        up_bias_sum,
    ) = lax.psum(
        (
            first_gain_gradient,
            first_shift_gradient,
            input_bias_gradient,
            output_bias_gradient,
            second_gain_gradient,
            second_shift_gradient,
            up_bias_gradient,
        ),
        ("fsdp", "context"),
    )
    input_sum, output_sum, up_sum, down_sum = (
        lax.psum_scatter(input_gradient, ("fsdp", "context"), scatter_dimension=0, tiled=True),
        lax.psum_scatter(output_gradient, ("fsdp", "context"), scatter_dimension=0, tiled=True),
        lax.psum_scatter(up_gradient, ("fsdp", "context"), scatter_dimension=0, tiled=True),
        lax.psum_scatter(down_gradient, ("fsdp", "context"), scatter_dimension=0, tiled=True),
    )
    return (
        block_output,
        tokens_gradient,
        first_gain_sum,
        first_shift_sum,
        input_sum,
        input_bias_sum,
        output_sum,
        output_bias_sum,
        second_gain_sum,
        second_shift_sum,
        up_sum,
        up_bias_sum,
        down_sum,
        clipped_weight,
        factor,
    )


def solution(mesh):
    placed = (
        P("fsdp", "context", None),
        P("fsdp", None),
        P(),
        P(),
        P(("fsdp", "context"), None, "tensor"),
        P(None, "tensor"),
        P(("fsdp", "context"), "tensor"),
        P(),
        P(),
        P(),
        P(("fsdp", "context"), "tensor"),
        P("tensor"),
        P(("fsdp", "context"), "tensor"),
        P("fsdp", "context", None),
    )
    chain = mesh.shape["fsdp"] // 2
    step = on_device
    if mesh.shape["context"] == 2 and mesh.shape["tensor"] == 2 and chain == 4:
        step = functools.partial(on_device_fused, chain=chain)
    return jax.shard_map(
        step,
        mesh=mesh,
        in_specs=placed,
        out_specs=(
            P("fsdp", "context", None),
            P("fsdp", "context", None),
            P(),
            P(),
            P(("fsdp", "context"), None, "tensor"),
            P(None, "tensor"),
            P(("fsdp", "context"), "tensor"),
            P(),
            P(),
            P(),
            P(("fsdp", "context"), "tensor"),
            P("tensor"),
            P(("fsdp", "context"), "tensor"),
            P(("fsdp", "context"), None, "tensor"),
            P("tensor"),
        ),
        check_vma=False,
    )
```
